32 devices in a mesh: dp: 1 (over z), tp: 4 (over y), sp: 8 (over x, core).
Axes of the slice: x: 4, y: 4, z: 1, core: 2. Of those that a mesh axis runs over, the one named last changes fastest.
The devices are a block of a 4x4x8 slice.
Arguments:
- x_in: bfloat16 [128, 6144], P('dp')
- positions: int32 [128], P('dp')
- k_cache: bfloat16 [128, 512, 8, 128], P('dp', 'sp', 'tp')
- v_cache: bfloat16 [128, 512, 8, 128], P('dp', 'sp', 'tp')
- attn_gain: bfloat16 [6144], replicated
- w_q: bfloat16 [6144, 6144], P(None, 'tp')
- w_k: bfloat16 [6144, 1024], P(None, 'tp')
- w_v: bfloat16 [6144, 1024], P(None, 'tp')
- w_o: bfloat16 [6144, 6144], P('tp')
- mlp_gain: bfloat16 [6144], replicated
- w_gate: bfloat16 [6144, 16384], P(None, ('tp', 'sp'))
- w_up: bfloat16 [6144, 16384], P(None, ('tp', 'sp'))
- w_down: bfloat16 [16384, 6144], P(('tp', 'sp'))
Outputs:
- output 1: bfloat16 [128, 6144], P('dp')
- output 2: bfloat16 [128, 512, 8, 128], P('dp', 'sp', 'tp')
- output 3: bfloat16 [128, 512, 8, 128], P('dp', 'sp', 'tp')
- output 4: bfloat16 [128, 8, 128], P('dp', 'tp')
- output 5: bfloat16 [128, 8, 128], P('dp', 'tp')
All inputs are finite; a program needn't handle non-finite values.
Results may differ from the reference program's by a relative error of at most 0.016995.
Values sent between devices are 32-bit elements.
A program may use at most 768 MiB of HBM per device.

```python
import math
import jax
import jax.numpy as jnp
from jax import lax

BATCH_ROWS = 128
CACHE_LEN = 512
MODEL_DIM = 6144
NUM_HEADS = 48
KV_HEADS = 8
HEAD_DIM = 128
FFN_DIM = 16384
ROPE_THETA = 1000000.0
NORM_EPS = 1e-05


def setup_inputs(seed: int = 0, part: int = 0) -> dict:
    base_key = jax.random.key(seed)
    shared_keys = jax.random.split(base_key, 9)
    part_keys = jax.random.split(jax.random.fold_in(base_key, part), 4)
    cache_shape = (BATCH_ROWS, CACHE_LEN, KV_HEADS, HEAD_DIM)
    q_width = NUM_HEADS * HEAD_DIM
    kv_width = KV_HEADS * HEAD_DIM
    x_in = jax.random.normal(part_keys[0], (BATCH_ROWS, MODEL_DIM), jnp.float32)
    positions = jax.random.randint(part_keys[1], (BATCH_ROWS,), CACHE_LEN // 2, CACHE_LEN, jnp.int32)
    positions = positions.at[0].set(CACHE_LEN - 1).at[1].set(CACHE_LEN // 2)
    k_cache = jax.random.normal(part_keys[2], cache_shape, jnp.float32)
    v_cache = jax.random.normal(part_keys[3], cache_shape, jnp.float32)
    attn_gain = 1.0 + 0.3 * jax.random.normal(shared_keys[0], (MODEL_DIM,), jnp.float32)
    w_q = jax.random.normal(shared_keys[1], (MODEL_DIM, q_width), jnp.float32) * (1.5 / math.sqrt(MODEL_DIM))
    w_k = jax.random.normal(shared_keys[2], (MODEL_DIM, kv_width), jnp.float32) / math.sqrt(MODEL_DIM)
    w_v = jax.random.normal(shared_keys[3], (MODEL_DIM, kv_width), jnp.float32) / math.sqrt(MODEL_DIM)
    w_o = jax.random.normal(shared_keys[4], (q_width, MODEL_DIM), jnp.float32) * (math.sqrt(CACHE_LEN / 16.0) / math.sqrt(q_width))
    mlp_gain = 1.0 + 0.3 * jax.random.normal(shared_keys[5], (MODEL_DIM,), jnp.float32)
    w_gate = jax.random.normal(shared_keys[6], (MODEL_DIM, FFN_DIM), jnp.float32) / math.sqrt(MODEL_DIM)
    w_up = jax.random.normal(shared_keys[7], (MODEL_DIM, FFN_DIM), jnp.float32) / math.sqrt(MODEL_DIM)
    w_down = jax.random.normal(shared_keys[8], (FFN_DIM, MODEL_DIM), jnp.float32) * (2.0 / math.sqrt(FFN_DIM))
    return {
        'x_in': x_in.astype(jnp.bfloat16),
        'positions': positions,
        'k_cache': k_cache.astype(jnp.bfloat16),
        'v_cache': v_cache.astype(jnp.bfloat16),
        'attn_gain': attn_gain.astype(jnp.bfloat16),
        'w_q': w_q.astype(jnp.bfloat16),
        'w_k': w_k.astype(jnp.bfloat16),
        'w_v': w_v.astype(jnp.bfloat16),
        'w_o': w_o.astype(jnp.bfloat16),
        'mlp_gain': mlp_gain.astype(jnp.bfloat16),
        'w_gate': w_gate.astype(jnp.bfloat16),
        'w_up': w_up.astype(jnp.bfloat16),
        'w_down': w_down.astype(jnp.bfloat16),
    }


def rms_norm(row_vals, gain_vec):
    vals32 = row_vals.astype(jnp.float32)
    inv_rms = lax.rsqrt(jnp.mean(vals32 * vals32, axis=-1, keepdims=True) + NORM_EPS)
    return (vals32 * inv_rms * gain_vec.astype(jnp.float32)).astype(jnp.bfloat16)


def apply_rotary(head_vecs, positions):
    half_dim = HEAD_DIM // 2
    inv_freq = ROPE_THETA ** (jnp.arange(half_dim, dtype=jnp.float32) * (-2.0 / HEAD_DIM))
    angles = positions.astype(jnp.float32)[:, None] * inv_freq[None, :]
    cos_part = jnp.cos(angles)[:, None, :]
    sin_part = jnp.sin(angles)[:, None, :]
    lower_half = head_vecs[..., :half_dim]
    upper_half = head_vecs[..., half_dim:]
    return jnp.concatenate([lower_half * cos_part - upper_half * sin_part, upper_half * cos_part + lower_half * sin_part], axis=-1)


def attend_row(row_data):
    q_row, k_row, v_row, pos_row = row_data
    scores = jnp.einsum('kgd,tkd->kgt', q_row.astype(jnp.float32), k_row.astype(jnp.float32)) * (HEAD_DIM ** -0.5)
    is_valid = jnp.arange(CACHE_LEN) <= pos_row
    scores = jnp.where(is_valid[None, None, :], scores, -jnp.inf)
    weights = jax.nn.softmax(scores, axis=-1)
    return jnp.einsum('kgt,tkd->kgd', weights, v_row.astype(jnp.float32))


def reference(x_in, positions, k_cache, v_cache, attn_gain, w_q, w_k, w_v, w_o, mlp_gain, w_gate, w_up, w_down):
    group_size = NUM_HEADS // KV_HEADS
    normed = rms_norm(x_in, attn_gain)
    q_proj = jnp.dot(normed, w_q, preferred_element_type=jnp.float32).astype(jnp.bfloat16)
    k_proj = jnp.dot(normed, w_k, preferred_element_type=jnp.float32).astype(jnp.bfloat16)
    v_new = jnp.dot(normed, w_v, preferred_element_type=jnp.float32).astype(jnp.bfloat16).reshape(BATCH_ROWS, KV_HEADS, HEAD_DIM)
    q_rot = apply_rotary(q_proj.astype(jnp.float32).reshape(BATCH_ROWS, NUM_HEADS, HEAD_DIM), positions).astype(jnp.bfloat16)
    k_new = apply_rotary(k_proj.astype(jnp.float32).reshape(BATCH_ROWS, KV_HEADS, HEAD_DIM), positions).astype(jnp.bfloat16)
    slot_hit = (jnp.arange(CACHE_LEN)[None, :] == positions[:, None])[:, :, None, None]
    k_out = jnp.where(slot_hit, k_new[:, None], k_cache)
    v_out = jnp.where(slot_hit, v_new[:, None], v_cache)
    q_grouped = q_rot.reshape(BATCH_ROWS, KV_HEADS, group_size, HEAD_DIM)
    attn_rows = lax.map(attend_row, (q_grouped, k_out, v_out, positions))
    attn_out = attn_rows.reshape(BATCH_ROWS, NUM_HEADS * HEAD_DIM).astype(jnp.bfloat16)
    x_mid = (x_in.astype(jnp.float32) + jnp.dot(attn_out, w_o, preferred_element_type=jnp.float32)).astype(jnp.bfloat16)
    normed_mlp = rms_norm(x_mid, mlp_gain)
    gate_val = jnp.dot(normed_mlp, w_gate, preferred_element_type=jnp.float32)
    up_val = jnp.dot(normed_mlp, w_up, preferred_element_type=jnp.float32)
    inner_act = (jax.nn.silu(gate_val) * up_val).astype(jnp.bfloat16)
    x_out = (x_mid.astype(jnp.float32) + jnp.dot(inner_act, w_down, preferred_element_type=jnp.float32)).astype(jnp.bfloat16)
    return (x_out, k_out, v_out, k_new, v_new)
```

```python
import functools

import jax
import jax.numpy as jnp
from jax import lax
from jax.experimental import pallas as pl
from jax.experimental.pallas import tpu as pltpu
from jax.sharding import PartitionSpec as P

ROPE_THETA = 1000000.0
NORM_EPS = 1e-05
MASK_FILL = -1.0e30
LANES = 128
SUBROWS = 8
CORES = 2
TILE = 512
MESH = pl.DeviceIdType.MESH
F32 = jnp.float32
BF16 = jnp.bfloat16


def rms_norm(row_vals, gain_vec):
    vals32 = row_vals.astype(F32)
    inv_rms = lax.rsqrt(jnp.mean(vals32 * vals32, axis=-1, keepdims=True) + NORM_EPS)
    return (vals32 * inv_rms * gain_vec.astype(F32)).astype(BF16)


def rotary_tables(positions, head_dim):
    half_dim = head_dim // 2
    inv_freq = ROPE_THETA ** (jnp.arange(half_dim, dtype=F32) * (-2.0 / head_dim))
    angles = positions.astype(F32)[:, None] * inv_freq[None, :]
    return jnp.cos(angles), jnp.sin(angles)


def apply_rotary(head_vecs, cos_part, sin_part):
    half_dim = head_vecs.shape[-1] // 2
    cos_part, sin_part = cos_part[:, None, :], sin_part[:, None, :]
    lower_half = head_vecs[..., :half_dim]
    upper_half = head_vecs[..., half_dim:]
    return jnp.concatenate([lower_half * cos_part - upper_half * sin_part, upper_half * cos_part + lower_half * sin_part], axis=-1)


def run_together(*flows):
    flows = list(flows)
    while flows:
        for flow in list(flows):
            if next(flow, flow) is flow:
                flows.remove(flow)


def merge_partials(left, right):
    width = left.shape[-1] - LANES
    stat_l, stat_r = left[:, width:], right[:, width:]
    lane = lax.broadcasted_iota(jnp.int32, stat_l.shape, 1)
    top = jnp.maximum(stat_l, stat_r)
    scale_l, scale_r = jnp.exp(stat_l - top), jnp.exp(stat_r - top)
    total = stat_l * pltpu.roll(scale_l, LANES // 2, 1) + stat_r * pltpu.roll(scale_r, LANES // 2, 1)
    parts = []
    for g in range(width // LANES):
        cols = slice(g * LANES, (g + 1) * LANES)
        parts.append(left[:, cols] * scale_l[:, g : g + 1] + right[:, cols] * scale_r[:, g : g + 1])
    parts.append(jnp.where(lane < LANES // 2, top, total))
    return jnp.concatenate(parts, axis=-1)


def rest_kernel(
    nx, ny, dim,
    part_ref, own_x_ref, gain_ref, wo_hbm, w1_hbm, w3_hbm, w2_hbm,
    out_ref,
    wo_v, w1_v, w3_v, w2_v, load_sem,
    pair_in, ring_a, ring_a_in, o_in, proj, proj_in, stat_out, stat_in,
    gathered, normed, other, other_in, mine, big_in, small_in, final,
    send_sem, recv_sem,
):
    sp, iy = lax.axis_index("sp"), lax.axis_index("tp")
    ix, core = sp // CORES, lax.rem(sp, CORES)
    half = wo_v.shape[1]
    heads_width = part_ref.shape[-1] - LANES

    def on_x(step):
        return lax.rem(ix + step + nx, nx)

    def on_y(step):
        return lax.rem(iy + step + ny, ny)

    partner = {"sp": ix * CORES + (1 - core)}
    x_right, x_left = {"sp": on_x(1) * CORES + core}, {"sp": on_x(-1) * CORES + core}
    y_right, y_left = {"tp": on_y(1)}, {"tp": on_y(-1)}

    loads = []

    def load(src, dst):
        copy = pltpu.make_async_copy(src, dst, load_sem.at[len(loads)])
        copy.start()
        loads.append(copy)
        return copy

    my_cols = pl.ds(pl.multiple_of(core * half, half), half)
    wo_load = load(wo_hbm.at[:, my_cols], wo_v)
    w1_load = load(w1_hbm, w1_v)
    w3_load = load(w3_hbm, w3_v)
    w2_load = load(w2_hbm, w2_v)

    barrier = pltpu.get_barrier_semaphore()
    peers = (partner, x_right, x_left, y_right, y_left)
    for peer in peers:
        pl.semaphore_signal(barrier, inc=1, device_id=peer, device_id_type=MESH)
    pl.semaphore_wait(barrier, len(peers))

    sent = []

    def send(src, dst, peer):
        k = len(sent)
        copy = pltpu.make_async_remote_copy(
            src_ref=src, dst_ref=dst, send_sem=send_sem.at[k], recv_sem=recv_sem.at[k], device_id=peer, device_id_type=MESH
        )
        copy.start()
        sent.append(copy)
        return copy

    def ring_reduce(piece, held, at, right, left, add, done):
        near_r, near_l, far = at(1), at(-1), at(2)
        r1 = send(piece(far, 0), held.at[0], right)
        l1 = send(piece(far, 1), held.at[1], left)
        r2 = send(piece(near_r, 1), held.at[2], right)
        l2 = send(piece(near_l, 0), held.at[3], left)
        yield
        r1.wait_recv()
        add(piece(near_r, 0), held.at[0])
        r3 = send(piece(near_r, 0), held.at[4], right)
        l1.wait_recv()
        add(piece(near_l, 1), held.at[1])
        l3 = send(piece(near_l, 1), held.at[5], left)
        yield
        me = at(0)
        l2.wait_recv()
        add(piece(me, 0), held.at[3])
        r2.wait_recv()
        add(piece(me, 1), held.at[2])
        yield
        r3.wait_recv()
        add(piece(me, 0), held.at[4])
        l3.wait_recv()
        add(piece(me, 1), held.at[5])
        done()

    def ring_gather(piece, at, right, left, arrived):
        me, from_l, from_r, far = at(0), at(-1), at(1), at(2)
        r1 = send(piece(me, 0), piece(me, 0), right)
        l1 = send(piece(me, 1), piece(me, 1), left)
        r2 = send(piece(me, 1), piece(me, 1), right)
        l2 = send(piece(me, 0), piece(me, 0), left)
        yield
        r1.wait_recv()
        r3 = send(piece(from_l, 0), piece(from_l, 0), right)
        arrived(piece(from_l, 0))
        l1.wait_recv()
        l3 = send(piece(from_r, 1), piece(from_r, 1), left)
        arrived(piece(from_r, 1))
        yield
        r2.wait_recv()
        arrived(piece(from_l, 1))
        l2.wait_recv()
        arrived(piece(from_r, 0))
        yield
        r3.wait_recv()
        arrived(piece(far, 0))
        l3.wait_recv()
        arrived(piece(far, 1))

    def add_into(dst, src):
        dst[...] = dst[...] + src[...]

    order = (on_x(2), on_x(1), on_x(-1), on_x(0))
    swaps = [send(part_ref.at[1 - core, t], pair_in.at[t], partner) for t in order]
    for t, swap in zip(order, swaps):
        swap.wait_recv()
        ring_a[t] = merge_partials(part_ref[core, t], pair_in[t])

    rows_half = ring_a.shape[1] // 2

    def part_piece(t, h):
        return ring_a.at[t, pl.ds(h * rows_half, rows_half)]

    def merge_into(dst, src):
        dst[...] = merge_partials(dst[...], src[...])

    run_together(ring_reduce(part_piece, ring_a_in, on_x, x_right, x_left, merge_into, lambda: None))
    merged = ring_a[on_x(0)]
    stats = merged[:, heads_width:]
    heads = []
    for g in range(heads_width // LANES):
        lsum = stats[:, LANES // 2 + g : LANES // 2 + g + 1]
        heads.append(merged[:, g * LANES : (g + 1) * LANES] / lsum)
    o_in[core] = jnp.concatenate(heads, axis=-1).astype(BF16).astype(F32)
    swap = send(o_in.at[core], o_in.at[core], partner)
    swap.wait_recv()
    attn = jnp.concatenate([o_in[c] for c in range(CORES)], axis=-1).astype(BF16)

    wo_load.wait()
    tiles = half // TILE
    for j in range(tiles):
        cols = slice(j * TILE, (j + 1) * TILE)
        prod = jnp.dot(attn, wo_v[:, cols], preferred_element_type=F32)
        proj[:, :, cols] = prod.reshape(ny, SUBROWS, TILE)

    def proj_piece(t, h):
        return proj.at[t, :, pl.ds(h * (half // 2), half // 2)]

    run_together(ring_reduce(proj_piece, proj_in, on_y, y_right, y_left, add_into, lambda: None))
    x_mid = (own_x_ref[...] + proj[iy]).astype(BF16).astype(F32)

    square = jnp.sum(x_mid * x_mid, axis=-1, keepdims=True)
    stat_out[...] = jnp.broadcast_to(square, stat_out.shape)
    swap = send(stat_out, stat_in, partner)
    swap.wait_recv()
    inv_rms = lax.rsqrt((stat_out[:, :1] + stat_in[:, :1]) / dim + NORM_EPS)
    gathered[core, ix, iy] = (x_mid * inv_rms * gain_ref[core]).astype(BF16).astype(F32)

    def gather_all(buf):
        quarter, eighth = half // 2, half // 4
        forwards = []

        def forward(ref_of):
            ref = ref_of(core)
            forwards.append(send(ref, ref, partner))

        def at(*index):
            return lambda c: buf.at[(c, *index)]

        forward(at(ix, iy))

        def flow(lo, y_first):
            def cols(h):
                return pl.ds(lo + h * eighth, eighth)

            def along_y_one(t, h):
                return buf.at[core, ix, t, :, cols(h)]

            def along_x_one(t, h):
                return buf.at[core, t, iy, :, cols(h)]

            def along_x_all(t, h):
                return buf.at[core, t, :, :, cols(h)]

            def along_y_all(t, h):
                return buf.at[core, :, t, :, cols(h)]

            def arrived(ref):
                forwards.append(send(ref, ref, partner))

            if y_first:
                yield from ring_gather(along_y_one, on_y, y_right, y_left, arrived)
                yield from ring_gather(along_x_all, on_x, x_right, x_left, arrived)
            else:
                yield from ring_gather(along_x_one, on_x, x_right, x_left, arrived)
                yield from ring_gather(along_y_all, on_y, y_right, y_left, arrived)

        run_together(flow(0, True), flow(quarter, False))
        for copy in forwards:
            copy.wait_recv()

    gather_all(gathered)
    rows = nx * ny * SUBROWS
    for c in range(CORES):
        normed[:, c * half : (c + 1) * half] = gathered[c].reshape(rows, half).astype(BF16)

    w1_load.wait()
    w3_load.wait()
    inner = w1_v.shape[1]
    step = 256
    acts = []
    for j in range(inner // step):
        cols = slice(j * step, (j + 1) * step)
        gate = jnp.dot(normed[...], w1_v[:, cols], preferred_element_type=F32)
        up = jnp.dot(normed[...], w3_v[:, cols], preferred_element_type=F32)
        acts.append((gate * jax.nn.sigmoid(gate) * up).astype(BF16))
    act = jnp.concatenate(acts, axis=-1)
    w2_load.wait()

    def down(which, j):
        cols = pl.ds(pl.multiple_of(which * half + j * TILE, TILE), TILE)
        return jnp.dot(act, w2_v[:, cols], preferred_element_type=F32).reshape(nx, ny, SUBROWS, TILE)

    swaps = []
    for j in range(tiles):
        cols = slice(j * TILE, (j + 1) * TILE)
        other[:, :, :, cols] = down(1 - core, j)
        swaps.append(send(other.at[:, :, :, cols], other_in.at[:, :, :, cols], partner))

    quarter, eighth = half // 2, half // 4

    def reduce_flow(index):
        lo = index * quarter

        def along_x_all(t, h):
            return mine.at[t, :, :, pl.ds(lo + h * eighth, eighth)]

        def along_y_all(t, h):
            return mine.at[:, t, :, pl.ds(lo + h * eighth, eighth)]

        def along_y_one(t, h):
            return mine.at[ix, t, :, pl.ds(lo + h * eighth, eighth)]

        def along_x_one(t, h):
            return mine.at[t, iy, :, pl.ds(lo + h * eighth, eighth)]

        for j in range(index * tiles // 2, (index + 1) * tiles // 2):
            cols = slice(j * TILE, (j + 1) * TILE)
            swaps[j].wait_recv()
            mine[:, :, :, cols] = down(core, j) + other_in[:, :, :, cols]
        if index == 0:
            yield from ring_reduce(along_x_all, big_in.at[0], on_x, x_right, x_left, add_into, lambda: None)
            yield from ring_reduce(along_y_one, small_in.at[0], on_y, y_right, y_left, add_into, lambda: None)
        else:
            yield from ring_reduce(along_y_all, big_in.at[1], on_y, y_right, y_left, add_into, lambda: None)
            yield from ring_reduce(along_x_one, small_in.at[1], on_x, x_right, x_left, add_into, lambda: None)

    run_together(reduce_flow(0), reduce_flow(1))
    final[core, ix, iy] = (x_mid + mine[ix, iy]).astype(BF16).astype(F32)
    gather_all(final)
    for c in range(CORES):
        out_ref[:, c * half : (c + 1) * half] = final[c].reshape(rows, half).astype(BF16)
    for copy in sent:
        copy.wait_send()


def rest_of_layer(mesh, parts, own_x, gain, w_o, w_gate, w_up, w_down):
    nx, ny = mesh.shape["sp"] // CORES, mesh.shape["tp"]
    dim = w_o.shape[1]
    half = dim // CORES
    rows = nx * ny * SUBROWS
    heads_width = parts.shape[-1] - LANES
    eighth = half // 4
    any_spec = pl.BlockSpec(memory_space=pltpu.HBM)
    vmem_spec = pl.BlockSpec(memory_space=pltpu.VMEM)
    width = heads_width + LANES
    chunk_rows = ny * SUBROWS
    count = 152
    scratch = [
        pltpu.VMEM((w_o.shape[0], half), BF16),
        pltpu.VMEM(w_gate.shape, BF16),
        pltpu.VMEM(w_up.shape, BF16),
        pltpu.VMEM(w_down.shape, BF16),
        pltpu.SemaphoreType.DMA((4,)),
        pltpu.VMEM((nx, chunk_rows, width), F32),
        pltpu.VMEM((nx, chunk_rows, width), F32),
        pltpu.VMEM((6, chunk_rows // 2, width), F32),
        pltpu.VMEM((CORES, chunk_rows, heads_width), F32),
        pltpu.VMEM((ny, SUBROWS, half), F32),
        pltpu.VMEM((6, SUBROWS, half // 2), F32),
        pltpu.VMEM((SUBROWS, LANES), F32),
        pltpu.VMEM((SUBROWS, LANES), F32),
        pltpu.VMEM((CORES, nx, ny, SUBROWS, half), F32),
        pltpu.VMEM((rows, dim), BF16),
        pltpu.VMEM((nx, ny, SUBROWS, half), F32),
        pltpu.VMEM((nx, ny, SUBROWS, half), F32),
        pltpu.VMEM((nx, ny, SUBROWS, half), F32),
        pltpu.VMEM((2, 6, nx, SUBROWS, eighth), F32),
        pltpu.VMEM((2, 6, SUBROWS, eighth), F32),
        pltpu.VMEM((CORES, nx, ny, SUBROWS, half), F32),
        pltpu.SemaphoreType.DMA((count,)),
        pltpu.SemaphoreType.DMA((count,)),
    ]
    return pl.pallas_call(
        functools.partial(rest_kernel, nx, ny, dim),
        out_shape=jax.ShapeDtypeStruct((rows, dim), BF16),
        in_specs=[vmem_spec] * 3 + [any_spec] * 4,
        out_specs=vmem_spec,
        scratch_shapes=scratch,
        compiler_params=pltpu.CompilerParams(collective_id=0, has_side_effects=True, vmem_limit_bytes=60 * 1024 * 1024),
        name="rest_of_layer",
    )(parts, own_x, gain, w_o, w_gate, w_up, w_down)


def solution(mesh):
    row_spec = P('dp', None)
    cache_spec = P('dp', 'sp', 'tp', None)
    new_spec = P('dp', 'tp', None)
    in_specs = (row_spec, P('dp'), cache_spec, cache_spec, P(None), P(None, 'tp'), P(None, 'tp'), P(None, 'tp'), P('tp', None), P(None), P(None, ('tp', 'sp')), P(None, ('tp', 'sp')), P(('tp', 'sp'), None))
    out_specs = (row_spec, cache_spec, cache_spec, new_spec, new_spec)
    nx, ny = mesh.shape["sp"] // CORES, mesh.shape["tp"]

    def local_step(x_in, positions, k_cache, v_cache, attn_gain, w_q, w_k, w_v, w_o, mlp_gain, w_gate, w_up, w_down):
        num_rows, block_len, kv_local, head_dim = k_cache.shape
        dim = x_in.shape[1]
        half = dim // CORES
        heads_local = w_q.shape[1] // head_dim
        group_size = heads_local // kv_local
        normed = rms_norm(x_in, attn_gain)
        q_proj = jnp.dot(normed, w_q, preferred_element_type=F32).astype(BF16)
        k_proj = jnp.dot(normed, w_k, preferred_element_type=F32).astype(BF16)
        v_new = jnp.dot(normed, w_v, preferred_element_type=F32).astype(BF16).reshape(num_rows, kv_local, head_dim)
        cos_part, sin_part = rotary_tables(positions, head_dim)
        q_rot = apply_rotary(q_proj.astype(F32).reshape(num_rows, heads_local, head_dim), cos_part, sin_part).astype(BF16)
        k_new = apply_rotary(k_proj.astype(F32).reshape(num_rows, kv_local, head_dim), cos_part, sin_part).astype(BF16)
        sp = lax.axis_index('sp')
        slot_ids = sp * block_len + jnp.arange(block_len)
        slot_hit = (slot_ids[None, :] == positions[:, None])[:, :, None, None]
        k_out = jnp.where(slot_hit, k_new[:, None], k_cache)
        v_out = jnp.where(slot_hit, v_new[:, None], v_cache)
        q_grouped = q_rot.reshape(num_rows, kv_local, group_size, head_dim)
        scores = jnp.einsum('bkgd,btkd->bkgt', q_grouped, k_out, preferred_element_type=F32) * (head_dim ** -0.5)
        is_valid = (slot_ids[None, :] <= positions[:, None])[:, None, None, :]
        scores = jnp.where(is_valid, scores, MASK_FILL)
        local_max = jnp.max(scores, axis=-1)
        weights = jnp.where(is_valid, jnp.exp(scores - local_max[..., None]), 0.0)
        local_sum = jnp.sum(weights, axis=-1)
        local_num = jnp.einsum('bkgt,btkd->bkgd', weights.astype(BF16), v_out, preferred_element_type=F32)
        gap = ((0, 0), (0, 0), (0, LANES // 2 - group_size))
        parts = jnp.concatenate([local_num.reshape(num_rows, kv_local, group_size * head_dim), jnp.pad(local_max, gap), jnp.pad(local_sum, gap)], axis=-1)
        parts = parts.transpose(1, 0, 2).reshape(kv_local, nx, num_rows // nx, -1)
        row0 = ((sp // CORES) * ny + lax.axis_index('tp')) * SUBROWS
        own_x = lax.dynamic_slice(x_in, (row0, lax.rem(sp, CORES) * half), (SUBROWS, half)).astype(F32)
        gain = mlp_gain.astype(F32).reshape(CORES, 1, half)
        x_out = rest_of_layer(mesh, parts, own_x, gain, w_o, w_gate, w_up, w_down)
        return x_out, k_out, v_out, k_new, v_new

    return jax.shard_map(local_step, mesh=mesh, in_specs=in_specs, out_specs=out_specs, check_vma=False)
```

```python
import functools

import jax
import jax.numpy as jnp
from jax import lax
from jax.experimental import pallas as pl
from jax.experimental.pallas import tpu as pltpu
from jax.sharding import PartitionSpec as P

ROPE_THETA = 1000000.0
NORM_EPS = 1e-05
MASK_FILL = -1.0e30
LANES = 128
SUBROWS = 8
CORES = 2
TILE = 512
MESH = pl.DeviceIdType.MESH
F32 = jnp.float32
BF16 = jnp.bfloat16


def rotary_tables(positions, head_dim):
    half_dim = head_dim // 2
    inv_freq = ROPE_THETA ** (jnp.arange(half_dim, dtype=F32) * (-2.0 / head_dim))
    angles = positions.astype(F32)[:, None] * inv_freq[None, :]
    cos_part, sin_part = jnp.cos(angles), jnp.sin(angles)
    return jnp.concatenate([cos_part, cos_part], axis=-1), jnp.concatenate([-sin_part, sin_part], axis=-1)


def run_together(*flows):
    flows = list(flows)
    while flows:
        for flow in list(flows):
            if next(flow, flow) is flow:
                flows.remove(flow)


def merge_partials(left, right):
    width = left.shape[-1] - LANES
    stat_l, stat_r = left[:, width:], right[:, width:]
    lane = lax.broadcasted_iota(jnp.int32, stat_l.shape, 1)
    top = jnp.maximum(stat_l, stat_r)
    scale_l, scale_r = jnp.exp(stat_l - top), jnp.exp(stat_r - top)
    total = stat_l * pltpu.roll(scale_l, LANES // 2, 1) + stat_r * pltpu.roll(scale_r, LANES // 2, 1)
    parts = []
    for g in range(width // LANES):
        cols = slice(g * LANES, (g + 1) * LANES)
        parts.append(left[:, cols] * scale_l[:, g : g + 1] + right[:, cols] * scale_r[:, g : g + 1])
    parts.append(jnp.where(lane < LANES // 2, top, total))
    return jnp.concatenate(parts, axis=-1)


def rest_kernel(
    nx, ny, dim,
    part_ref, gain_ref, x_hbm, wo_hbm, w1_hbm, w3_hbm, w2_hbm,
    out_ref,
    own_x, wo_v, w1_v, w3_v, w2_v, load_sem,
    pair_in, ring_a, ring_a_in, o_in, proj, proj_in, stat_out, stat_in,
    gathered, normed, other, other_in, mine, big_in, small_in, final,
    send_sem, recv_sem,
):
    sp, iy = lax.axis_index("sp"), lax.axis_index("tp")
    ix, core = sp // CORES, lax.rem(sp, CORES)
    half = wo_v.shape[1]
    heads_width = part_ref.shape[-1] - LANES

    def on_x(step):
        return lax.rem(ix + step + nx, nx)

    def on_y(step):
        return lax.rem(iy + step + ny, ny)

    partner = {"sp": ix * CORES + (1 - core)}
    x_right, x_left = {"sp": on_x(1) * CORES + core}, {"sp": on_x(-1) * CORES + core}
    y_right, y_left = {"tp": on_y(1)}, {"tp": on_y(-1)}

    loads = []

    def load(src, dst):
        copy = pltpu.make_async_copy(src, dst, load_sem.at[len(loads)])
        copy.start()
        loads.append(copy)
        return copy

    my_cols = pl.ds(pl.multiple_of(core * half, half), half)
    x_load = load(x_hbm.at[ix * ny + iy, :, my_cols], own_x)
    wo_load = load(wo_hbm.at[:, my_cols], wo_v)
    w1_load = load(w1_hbm, w1_v)
    w3_load = load(w3_hbm, w3_v)
    w2_load = load(w2_hbm, w2_v)

    barrier = pltpu.get_barrier_semaphore()
    peers = (partner, x_right, x_left, y_right, y_left)
    for peer in peers:
        pl.semaphore_signal(barrier, inc=1, device_id=peer, device_id_type=MESH)
    pl.semaphore_wait(barrier, len(peers))

    sent = []

    def send(src, dst, peer):
        k = len(sent)
        copy = pltpu.make_async_remote_copy(
            src_ref=src, dst_ref=dst, send_sem=send_sem.at[k], recv_sem=recv_sem.at[k], device_id=peer, device_id_type=MESH
        )
        copy.start()
        sent.append(copy)
        return copy

    def ring_reduce(piece, held, at, right, left, add, done):
        near_r, near_l, far = at(1), at(-1), at(2)
        r1 = send(piece(far, 0), held.at[0], right)
        l1 = send(piece(far, 1), held.at[1], left)
        r2 = send(piece(near_r, 1), held.at[2], right)
        l2 = send(piece(near_l, 0), held.at[3], left)
        yield
        r1.wait_recv()
        add(piece(near_r, 0), held.at[0])
        r3 = send(piece(near_r, 0), held.at[4], right)
        l1.wait_recv()
        add(piece(near_l, 1), held.at[1])
        l3 = send(piece(near_l, 1), held.at[5], left)
        yield
        me = at(0)
        l2.wait_recv()
        add(piece(me, 0), held.at[3])
        r2.wait_recv()
        add(piece(me, 1), held.at[2])
        yield
        r3.wait_recv()
        add(piece(me, 0), held.at[4])
        l3.wait_recv()
        add(piece(me, 1), held.at[5])
        done()

    def ring_gather(piece, at, right, left, arrived):
        me, from_l, from_r, far = at(0), at(-1), at(1), at(2)
        r1 = send(piece(me, 0), piece(me, 0), right)
        l1 = send(piece(me, 1), piece(me, 1), left)
        r2 = send(piece(me, 1), piece(me, 1), right)
        l2 = send(piece(me, 0), piece(me, 0), left)
        yield
        r1.wait_recv()
        r3 = send(piece(from_l, 0), piece(from_l, 0), right)
        arrived(piece(from_l, 0))
        l1.wait_recv()
        l3 = send(piece(from_r, 1), piece(from_r, 1), left)
        arrived(piece(from_r, 1))
        yield
        r2.wait_recv()
        arrived(piece(from_l, 1))
        l2.wait_recv()
        arrived(piece(from_r, 0))
        yield
        r3.wait_recv()
        arrived(piece(far, 0))
        l3.wait_recv()
        arrived(piece(far, 1))

    def add_into(dst, src):
        dst[...] = dst[...] + src[...]

    order = (on_x(2), on_x(1), on_x(-1), on_x(0))
    swaps = [send(part_ref.at[1 - core, t], pair_in.at[t], partner) for t in order]
    for t, swap in zip(order, swaps):
        swap.wait_recv()
        ring_a[t] = merge_partials(part_ref[core, t], pair_in[t])

    rows_half = ring_a.shape[1] // 2

    def part_piece(t, h):
        return ring_a.at[t, pl.ds(h * rows_half, rows_half)]

    def merge_into(dst, src):
        dst[...] = merge_partials(dst[...], src[...])

    run_together(ring_reduce(part_piece, ring_a_in, on_x, x_right, x_left, merge_into, lambda: None))
    merged = ring_a[on_x(0)]
    stats = merged[:, heads_width:]
    heads = []
    for g in range(heads_width // LANES):
        lsum = stats[:, LANES // 2 + g : LANES // 2 + g + 1]
        heads.append(merged[:, g * LANES : (g + 1) * LANES] / lsum)
    o_in[core] = jnp.concatenate(heads, axis=-1).astype(BF16).astype(F32)
    swap = send(o_in.at[core], o_in.at[core], partner)
    swap.wait_recv()
    attn = jnp.concatenate([o_in[c] for c in range(CORES)], axis=-1).astype(BF16)

    wo_load.wait()
    tiles = half // TILE
    for j in range(tiles):
        cols = slice(j * TILE, (j + 1) * TILE)
        prod = jnp.dot(attn, wo_v[:, cols], preferred_element_type=F32)
        proj[:, :, cols] = prod.reshape(ny, SUBROWS, TILE)

    def proj_piece(t, h):
        return proj.at[t, :, pl.ds(h * (half // 2), half // 2)]

    run_together(ring_reduce(proj_piece, proj_in, on_y, y_right, y_left, add_into, lambda: None))
    x_load.wait()
    x_mid = (own_x[...].astype(F32) + proj[iy]).astype(BF16).astype(F32)

    square = jnp.sum(x_mid * x_mid, axis=-1, keepdims=True)
    stat_out[...] = jnp.broadcast_to(square, stat_out.shape)
    swap = send(stat_out, stat_in, partner)
    swap.wait_recv()
    inv_rms = lax.rsqrt((stat_out[:, :1] + stat_in[:, :1]) / dim + NORM_EPS)
    gathered[core, ix, iy] = (x_mid * inv_rms * gain_ref[core]).astype(BF16).astype(F32)

    def gather_all(buf):
        quarter, eighth = half // 2, half // 4
        forwards = []

        def forward(ref_of):
            ref = ref_of(core)
            forwards.append(send(ref, ref, partner))

        def at(*index):
            return lambda c: buf.at[(c, *index)]

        forward(at(ix, iy))

        def flow(lo, y_first):
            def cols(h):
                return pl.ds(lo + h * eighth, eighth)

            def along_y_one(t, h):
                return buf.at[core, ix, t, :, cols(h)]

            def along_x_one(t, h):
                return buf.at[core, t, iy, :, cols(h)]

            def along_x_all(t, h):
                return buf.at[core, t, :, :, cols(h)]

            def along_y_all(t, h):
                return buf.at[core, :, t, :, cols(h)]

            def arrived(ref):
                forwards.append(send(ref, ref, partner))

            if y_first:
                yield from ring_gather(along_y_one, on_y, y_right, y_left, arrived)
                yield from ring_gather(along_x_all, on_x, x_right, x_left, arrived)
            else:
                yield from ring_gather(along_x_one, on_x, x_right, x_left, arrived)
                yield from ring_gather(along_y_all, on_y, y_right, y_left, arrived)

        run_together(flow(0, True), flow(quarter, False))
        for copy in forwards:
            copy.wait_recv()

    gather_all(gathered)
    rows = nx * ny * SUBROWS
    for c in range(CORES):
        normed[:, c * half : (c + 1) * half] = gathered[c].reshape(rows, half).astype(BF16)

    w1_load.wait()
    w3_load.wait()
    inner = w1_v.shape[1]
    step = 256
    acts = []
    for j in range(inner // step):
        cols = slice(j * step, (j + 1) * step)
        gate = jnp.dot(normed[...], w1_v[:, cols], preferred_element_type=F32)
        up = jnp.dot(normed[...], w3_v[:, cols], preferred_element_type=F32)
        acts.append((gate * jax.nn.sigmoid(gate) * up).astype(BF16))
    act = jnp.concatenate(acts, axis=-1)
    w2_load.wait()

    def down(which, j):
        cols = pl.ds(pl.multiple_of(which * half + j * TILE, TILE), TILE)
        return jnp.dot(act, w2_v[:, cols], preferred_element_type=F32).reshape(nx, ny, SUBROWS, TILE)

    swaps = []
    for j in range(tiles):
        cols = slice(j * TILE, (j + 1) * TILE)
        other[:, :, :, cols] = down(1 - core, j)
        swaps.append(send(other.at[:, :, :, cols], other_in.at[:, :, :, cols], partner))

    quarter, eighth = half // 2, half // 4

    def reduce_flow(index):
        lo = index * quarter

        def along_x_all(t, h):
            return mine.at[t, :, :, pl.ds(lo + h * eighth, eighth)]

        def along_y_all(t, h):
            return mine.at[:, t, :, pl.ds(lo + h * eighth, eighth)]

        def along_y_one(t, h):
            return mine.at[ix, t, :, pl.ds(lo + h * eighth, eighth)]

        def along_x_one(t, h):
            return mine.at[t, iy, :, pl.ds(lo + h * eighth, eighth)]

        for j in range(index * tiles // 2, (index + 1) * tiles // 2):
            cols = slice(j * TILE, (j + 1) * TILE)
            swaps[j].wait_recv()
            mine[:, :, :, cols] = down(core, j) + other_in[:, :, :, cols]
        if index == 0:
            yield from ring_reduce(along_x_all, big_in.at[0], on_x, x_right, x_left, add_into, lambda: None)
            yield from ring_reduce(along_y_one, small_in.at[0], on_y, y_right, y_left, add_into, lambda: None)
        else:
            yield from ring_reduce(along_y_all, big_in.at[1], on_y, y_right, y_left, add_into, lambda: None)
            yield from ring_reduce(along_x_one, small_in.at[1], on_x, x_right, x_left, add_into, lambda: None)

    run_together(reduce_flow(0), reduce_flow(1))
    final[core, ix, iy] = (x_mid + mine[ix, iy]).astype(BF16).astype(F32)
    gather_all(final)
    for c in range(CORES):
        out_ref[:, c * half : (c + 1) * half] = final[c].reshape(rows, half).astype(BF16)
    for copy in sent:
        copy.wait_send()


def front_kernel(
    group_size, kv_local,
    x_ref, gain_ref, cos_ref, sin_ref, pos_ref, wq_hbm, wk_hbm, wv_hbm, k_hbm, v_hbm,
    parts_ref, k_out_hbm, v_out_hbm, k_new_ref, v_new_ref,
    wq_v, wk_v, wv_v, k_buf, v_buf, normed, q_rows, num_rows, max_rows, sum_rows, k_rows, v_rows,
    load_sem, store_sem,
):
    rows, dim = x_ref.shape
    columns = k_buf.shape[1]
    block_len = columns // kv_local
    head_dim = k_buf.shape[2]
    slots = SUBROWS * kv_local
    first_slot = lax.axis_index("sp") * block_len
    scale = head_dim ** -0.5

    loads = []

    def load(src, dst):
        copy = pltpu.make_async_copy(src, dst, load_sem.at[len(loads)])
        copy.start()
        loads.append(copy)
        return copy

    step = 2 * head_dim
    q_steps = wq_v.shape[1] // step
    early = q_steps // 2
    wk_load = load(wk_hbm, wk_v)
    wv_load = load(wv_hbm, wv_v)
    q_loads = [load(wq_hbm.at[:, pl.ds(j * step, step)], wq_v.at[:, pl.ds(j * step, step)]) for j in range(early)]
    k_load = load(k_hbm, k_buf)
    v_load = load(v_hbm, v_buf)
    q_loads += [load(wq_hbm.at[:, pl.ds(j * step, step)], wq_v.at[:, pl.ds(j * step, step)]) for j in range(early, q_steps)]

    q_rows[...] = jnp.zeros_like(q_rows)
    block = 2 * SUBROWS

    @pl.loop(0, rows // block)
    def _(i):
        at = pl.ds(pl.multiple_of(i * block, block), block)
        vals = x_ref[at, :].astype(F32)
        inv_rms = lax.rsqrt(jnp.mean(vals * vals, axis=-1, keepdims=True) + NORM_EPS)
        normed[at, :] = (vals * inv_rms * gain_ref[...]).astype(BF16)

    def rotate(vals):
        vals = vals.astype(BF16).astype(F32)
        return (vals * cos_ref[...] + pltpu.roll(vals, head_dim // 2, 1) * sin_ref[...]).astype(BF16)

    wk_load.wait()
    k_proj = jnp.dot(normed[...], wk_v[...], preferred_element_type=F32)
    for k in range(kv_local):
        cols = slice(k * head_dim, (k + 1) * head_dim)
        rotated = rotate(k_proj[:, cols])
        k_new_ref[:, cols] = rotated
        k_rows[pl.ds(k, rows, stride=kv_local), :] = rotated.astype(F32)
    wv_load.wait()
    v_proj = jnp.dot(normed[...], wv_v[...], preferred_element_type=F32).astype(BF16)
    v_new_ref[...] = v_proj
    for k in range(kv_local):
        v_rows[pl.ds(k, rows, stride=kv_local), :] = v_proj[:, k * head_dim : (k + 1) * head_dim].astype(F32)

    def project(j):
        q_loads[j].wait()
        prod = jnp.dot(normed[...], wq_v[:, j * step : (j + 1) * step], preferred_element_type=F32)
        for n in range(step // head_dim):
            head = j * (step // head_dim) + n
            row = head // group_size * SUBROWS + head % group_size
            q_rows[pl.ds(row, rows, stride=slots), :] = rotate(prod[:, n * head_dim : (n + 1) * head_dim]).astype(F32)

    for j in range(early + 1):
        project(j)
    k_load.wait()
    v_load.wait()
    sub = lax.broadcasted_iota(jnp.int32, (block, head_dim), 0)
    per_block = block // kv_local

    @pl.loop(0, rows)
    def _(b):
        p = pos_ref[b] - first_slot

        @pl.when((p >= 0) & (p < block_len))
        def _():
            at = pl.ds(pl.multiple_of(p // per_block * block, block), block)
            hit = sub // kv_local == p % per_block
            for buf, new_rows in ((k_buf, k_rows), (v_buf, v_rows)):
                new = new_rows[pl.ds(b * kv_local, 1), :]
                for k in range(1, kv_local):
                    new = jnp.where(sub % kv_local == k, new_rows[pl.ds(b * kv_local + k, 1), :], new)
                buf[b, at, :] = jnp.where(hit, new, buf[b, at, :].astype(F32)).astype(BF16)

    for j in range(early + 1, q_steps):
        project(j)
    stores = [
        pltpu.make_async_copy(k_buf, k_out_hbm, store_sem.at[0]),
        pltpu.make_async_copy(v_buf, v_out_hbm, store_sem.at[1]),
    ]
    for store in stores:
        store.start()

    col = lax.broadcasted_iota(jnp.int32, (slots, columns), 1)
    own_head = col % kv_local == lax.broadcasted_iota(jnp.int32, (slots, columns), 0) // SUBROWS
    time = jnp.where(own_head, first_slot + col // kv_local, jnp.iinfo(jnp.int32).max)
    together = SUBROWS

    @pl.loop(0, rows // together)
    def _(i):
        for u in range(together):
            b = i * together + u
            at = pl.ds(pl.multiple_of(b * slots, slots), slots)
            scores = lax.dot_general(q_rows[at, :].astype(BF16), k_buf[b], (((1,), (1,)), ((), ())), preferred_element_type=F32) * scale
            valid = time <= pos_ref[b]
            scores = jnp.where(valid, scores, MASK_FILL)
            top = jnp.max(scores, axis=-1, keepdims=True)
            weights = jnp.where(valid, jnp.exp(scores - top), 0.0)
            total = jnp.sum(weights, axis=-1, keepdims=True)
            num_rows[at, :] = jnp.dot(weights.astype(BF16), v_buf[b], preferred_element_type=F32)
            max_rows[at, :] = jnp.broadcast_to(top, (slots, LANES))
            sum_rows[at, :] = jnp.broadcast_to(total, (slots, LANES))

    lane = lax.broadcasted_iota(jnp.int32, (rows, LANES), 1)
    width = group_size * head_dim
    for k in range(kv_local):
        stats = jnp.zeros((rows, LANES), F32)
        for g in range(group_size):
            at = pl.ds(k * SUBROWS + g, rows, stride=slots)
            parts_ref[k, :, g * head_dim : (g + 1) * head_dim] = num_rows[at, :]
            stats = jnp.where(lane == g, max_rows[at, :], stats)
            stats = jnp.where(lane == LANES // 2 + g, sum_rows[at, :], stats)
        parts_ref[k, :, width:] = stats
    for store in stores:
        store.wait()


def front_of_layer(x_in, gain, cos_part, sin_part, positions, w_q, w_k, w_v, k_flat, v_flat, kv_local):
    rows, dim = x_in.shape
    columns, head_dim = k_flat.shape[1:]
    group_size = w_q.shape[1] // head_dim // kv_local
    assert group_size <= SUBROWS
    slots = SUBROWS * kv_local
    hbm_spec = pl.BlockSpec(memory_space=pltpu.HBM)
    vmem_spec = pl.BlockSpec(memory_space=pltpu.VMEM)
    smem_spec = pl.BlockSpec(memory_space=pltpu.SMEM)
    kv_width = w_k.shape[1]
    row_buf = pltpu.VMEM((rows * slots, LANES), F32)
    new_buf = pltpu.VMEM((rows * kv_local, head_dim), F32)
    return pl.pallas_call(
        functools.partial(front_kernel, group_size, kv_local),
        out_shape=(
            jax.ShapeDtypeStruct((kv_local, rows, group_size * head_dim + LANES), F32),
            jax.ShapeDtypeStruct(k_flat.shape, BF16),
            jax.ShapeDtypeStruct(v_flat.shape, BF16),
            jax.ShapeDtypeStruct((rows, kv_width), BF16),
            jax.ShapeDtypeStruct((rows, kv_width), BF16),
        ),
        in_specs=[vmem_spec] * 4 + [smem_spec] + [hbm_spec] * 5,
        out_specs=(vmem_spec, hbm_spec, hbm_spec, vmem_spec, vmem_spec),
        scratch_shapes=[
            pltpu.VMEM(w_q.shape, BF16),
            pltpu.VMEM(w_k.shape, BF16),
            pltpu.VMEM(w_v.shape, BF16),
            pltpu.VMEM(k_flat.shape, BF16),
            pltpu.VMEM(v_flat.shape, BF16),
            pltpu.VMEM(x_in.shape, BF16),
            row_buf, row_buf, row_buf, row_buf, new_buf, new_buf,
            pltpu.SemaphoreType.DMA((w_q.shape[1] // (2 * head_dim) + 4,)),
            pltpu.SemaphoreType.DMA((2,)),
        ],
        compiler_params=pltpu.CompilerParams(vmem_limit_bytes=56 * 1024 * 1024),
        name="front_of_layer",
    )(x_in, gain, cos_part, sin_part, positions, w_q, w_k, w_v, k_flat, v_flat)


def rest_of_layer(mesh, parts, own_x, gain, w_o, w_gate, w_up, w_down):
    nx, ny = mesh.shape["sp"] // CORES, mesh.shape["tp"]
    dim = w_o.shape[1]
    half = dim // CORES
    rows = nx * ny * SUBROWS
    heads_width = parts.shape[-1] - LANES
    eighth = half // 4
    any_spec = pl.BlockSpec(memory_space=pltpu.HBM)
    vmem_spec = pl.BlockSpec(memory_space=pltpu.VMEM)
    width = heads_width + LANES
    chunk_rows = ny * SUBROWS
    count = 152
    scratch = [
        pltpu.VMEM((SUBROWS, half), BF16),
        pltpu.VMEM((w_o.shape[0], half), BF16),
        pltpu.VMEM(w_gate.shape, BF16),
        pltpu.VMEM(w_up.shape, BF16),
        pltpu.VMEM(w_down.shape, BF16),
        pltpu.SemaphoreType.DMA((5,)),
        pltpu.VMEM((nx, chunk_rows, width), F32),
        pltpu.VMEM((nx, chunk_rows, width), F32),
        pltpu.VMEM((6, chunk_rows // 2, width), F32),
        pltpu.VMEM((CORES, chunk_rows, heads_width), F32),
        pltpu.VMEM((ny, SUBROWS, half), F32),
        pltpu.VMEM((6, SUBROWS, half // 2), F32),
        pltpu.VMEM((SUBROWS, LANES), F32),
        pltpu.VMEM((SUBROWS, LANES), F32),
        pltpu.VMEM((CORES, nx, ny, SUBROWS, half), F32),
        pltpu.VMEM((rows, dim), BF16),
        pltpu.VMEM((nx, ny, SUBROWS, half), F32),
        pltpu.VMEM((nx, ny, SUBROWS, half), F32),
        pltpu.VMEM((nx, ny, SUBROWS, half), F32),
        pltpu.VMEM((2, 6, nx, SUBROWS, eighth), F32),
        pltpu.VMEM((2, 6, SUBROWS, eighth), F32),
        pltpu.VMEM((CORES, nx, ny, SUBROWS, half), F32),
        pltpu.SemaphoreType.DMA((count,)),
        pltpu.SemaphoreType.DMA((count,)),
    ]
    return pl.pallas_call(
        functools.partial(rest_kernel, nx, ny, dim),
        out_shape=jax.ShapeDtypeStruct((rows, dim), BF16),
        in_specs=[vmem_spec] * 2 + [any_spec] * 5,
        out_specs=vmem_spec,
        scratch_shapes=scratch,
        compiler_params=pltpu.CompilerParams(collective_id=0, has_side_effects=True, vmem_limit_bytes=60 * 1024 * 1024),
        name="rest_of_layer",
    )(parts, gain, own_x, w_o, w_gate, w_up, w_down)


def solution(mesh):
    row_spec = P('dp', None)
    cache_spec = P('dp', 'sp', 'tp', None)
    new_spec = P('dp', 'tp', None)
    in_specs = (row_spec, P('dp'), cache_spec, cache_spec, P(None), P(None, 'tp'), P(None, 'tp'), P(None, 'tp'), P('tp', None), P(None), P(None, ('tp', 'sp')), P(None, ('tp', 'sp')), P(('tp', 'sp'), None))
    out_specs = (row_spec, cache_spec, cache_spec, new_spec, new_spec)
    nx, ny = mesh.shape["sp"] // CORES, mesh.shape["tp"]

    def local_step(x_in, positions, k_cache, v_cache, attn_gain, w_q, w_k, w_v, w_o, mlp_gain, w_gate, w_up, w_down):
        num_rows, block_len, kv_local, head_dim = k_cache.shape
        dim = x_in.shape[1]
        half = dim // CORES
        cos_part, sin_part = rotary_tables(positions, head_dim)
        flat = (num_rows, block_len * kv_local, head_dim)
        parts, k_out, v_out, k_new, v_new = front_of_layer(
            x_in, attn_gain.astype(F32)[None, :], cos_part, sin_part, positions, w_q, w_k, w_v,
            k_cache.reshape(flat), v_cache.reshape(flat), kv_local,
        )
        k_out, v_out = k_out.reshape(k_cache.shape), v_out.reshape(v_cache.shape)
        k_new, v_new = k_new.reshape(num_rows, kv_local, head_dim), v_new.reshape(num_rows, kv_local, head_dim)
        parts = parts.reshape(kv_local, nx, num_rows // nx, parts.shape[-1])
        own_x = x_in.reshape(nx * ny, SUBROWS, dim)
        gain = mlp_gain.astype(F32).reshape(CORES, 1, half)
        x_out = rest_of_layer(mesh, parts, own_x, gain, w_o, w_gate, w_up, w_down)
        return x_out, k_out, v_out, k_new, v_new

    return jax.shard_map(local_step, mesh=mesh, in_specs=in_specs, out_specs=out_specs, check_vma=False)
```

```python
import functools

import jax
import jax.numpy as jnp
from jax import lax
from jax.experimental import pallas as pl
from jax.experimental.pallas import tpu as pltpu
from jax.sharding import PartitionSpec as P

ROPE_THETA = 1000000.0
NORM_EPS = 1e-05
MASK_FILL = -1.0e30
LANES = 128
SUBROWS = 8
CORES = 2
TILE = 512
MESH = pl.DeviceIdType.MESH
F32 = jnp.float32
BF16 = jnp.bfloat16


def rotary_tables(positions, head_dim):
    half_dim = head_dim // 2
    inv_freq = ROPE_THETA ** (jnp.arange(half_dim, dtype=F32) * (-2.0 / head_dim))
    angles = positions.astype(F32)[:, None] * inv_freq[None, :]
    cos_part, sin_part = jnp.cos(angles), jnp.sin(angles)
    return jnp.concatenate([cos_part, cos_part], axis=-1), jnp.concatenate([-sin_part, sin_part], axis=-1)


def run_together(*flows):
    flows = list(flows)
    while flows:
        for flow in list(flows):
            if next(flow, flow) is flow:
                flows.remove(flow)


def merge_partials(left, right):
    width = left.shape[-1] - LANES
    stat_l, stat_r = left[:, width:], right[:, width:]
    lane = lax.broadcasted_iota(jnp.int32, stat_l.shape, 1)
    top = jnp.maximum(stat_l, stat_r)
    scale_l, scale_r = jnp.exp(stat_l - top), jnp.exp(stat_r - top)
    total = stat_l * pltpu.roll(scale_l, LANES // 2, 1) + stat_r * pltpu.roll(scale_r, LANES // 2, 1)
    parts = []
    for g in range(width // LANES):
        cols = slice(g * LANES, (g + 1) * LANES)
        parts.append(left[:, cols] * scale_l[:, g : g + 1] + right[:, cols] * scale_r[:, g : g + 1])
    parts.append(jnp.where(lane < LANES // 2, top, total))
    return jnp.concatenate(parts, axis=-1)


def rest_kernel(
    nx, ny, dim,
    part_ref, gain_ref, x_ref, wo_hbm, w1_hbm, w3_hbm, w2_hbm,
    out_ref,
    wo_v, w1_v, w3_v, w2_v, load_sem,
    pair_in, ring_a, ring_a_in, o_in, proj, proj_in, stat_out, stat_in,
    gathered, normed, other, other_in, mine, big_in, small_in, final,
    send_sem, recv_sem,
):
    sp, iy = lax.axis_index("sp"), lax.axis_index("tp")
    ix, core = sp // CORES, lax.rem(sp, CORES)
    half = wo_v.shape[1]
    heads_width = part_ref.shape[-1] - LANES

    def on_x(step):
        return lax.rem(ix + step + nx, nx)

    def on_y(step):
        return lax.rem(iy + step + ny, ny)

    partner = {"sp": ix * CORES + (1 - core)}
    x_right, x_left = {"sp": on_x(1) * CORES + core}, {"sp": on_x(-1) * CORES + core}
    y_right, y_left = {"tp": on_y(1)}, {"tp": on_y(-1)}

    loads = []

    def load(src, dst):
        copy = pltpu.make_async_copy(src, dst, load_sem.at[len(loads)])
        copy.start()
        loads.append(copy)
        return copy

    my_cols = pl.ds(pl.multiple_of(core * half, half), half)
    wo_load = load(wo_hbm.at[:, my_cols], wo_v)
    w1_load = load(w1_hbm, w1_v)
    w3_load = load(w3_hbm, w3_v)
    w2_load = load(w2_hbm, w2_v)

    barrier = pltpu.get_barrier_semaphore()
    peers = (partner, x_right, x_left, y_right, y_left)
    for peer in peers:
        pl.semaphore_signal(barrier, inc=1, device_id=peer, device_id_type=MESH)
    pl.semaphore_wait(barrier, len(peers))

    sent = []

    def send(src, dst, peer):
        k = len(sent)
        copy = pltpu.make_async_remote_copy(
            src_ref=src, dst_ref=dst, send_sem=send_sem.at[k], recv_sem=recv_sem.at[k], device_id=peer, device_id_type=MESH
        )
        copy.start()
        sent.append(copy)
        return copy

    on_ring_x, on_ring_y = (on_x, x_right, x_left), (on_y, y_right, y_left)

    def reduce_begin(piece, held, ring, add):
        at, right, left = ring
        r1 = send(piece(at(2), 0), held.at[0], right)
        l1 = send(piece(at(2), 1), held.at[1], left)
        r2 = send(piece(at(1), 1), held.at[2], right)
        l2 = send(piece(at(-1), 0), held.at[3], left)
        return [piece, held, ring, add, r1, l1, r2, l2]

    def reduce_turn(state):
        piece, held, (at, right, left), add, r1, l1 = state[:6]
        r1.wait_recv()
        add(piece(at(1), 0), held.at[0])
        state.append(send(piece(at(1), 0), held.at[4], right))
        l1.wait_recv()
        add(piece(at(-1), 1), held.at[1])
        state.append(send(piece(at(-1), 1), held.at[5], left))

    def reduce_end(state):
        piece, held, (at, _, _), add, _, _, r2, l2, r3, l3 = state
        for copy, h, k in ((l2, 0, 3), (r2, 1, 2), (r3, 0, 4), (l3, 1, 5)):
            copy.wait_recv()
            add(piece(at(0), h), held.at[k])

    def reduce_all(piece, held, ring, add):
        state = reduce_begin(piece, held, ring, add)
        reduce_turn(state)
        reduce_end(state)

    def add_into(dst, src):
        dst[...] = dst[...] + src[...]

    order = (on_x(2), on_x(1), on_x(-1), on_x(0))
    swaps = [send(part_ref.at[1 - core, t], pair_in.at[t], partner) for t in order]
    for t, swap in zip(order, swaps):
        swap.wait_recv()
        ring_a[t] = merge_partials(part_ref[core, t], pair_in[t])

    rows_half = ring_a.shape[1] // 2

    def part_piece(t, h):
        return ring_a.at[t, pl.ds(h * rows_half, rows_half)]

    def merge_into(dst, src):
        dst[...] = merge_partials(dst[...], src[...])

    reduce_all(part_piece, ring_a_in, on_ring_x, merge_into)
    merged = ring_a[on_x(0)]
    stats = merged[:, heads_width:]
    heads = []
    for g in range(heads_width // LANES):
        lsum = stats[:, LANES // 2 + g : LANES // 2 + g + 1]
        heads.append(merged[:, g * LANES : (g + 1) * LANES] / lsum)
    o_in[core] = jnp.concatenate(heads, axis=-1).astype(BF16).astype(F32)
    swap = send(o_in.at[core], o_in.at[core], partner)
    swap.wait_recv()
    attn = jnp.concatenate([o_in[c] for c in range(CORES)], axis=-1).astype(BF16)

    wo_load.wait()
    tiles = half // TILE
    for j in range(tiles):
        cols = slice(j * TILE, (j + 1) * TILE)
        prod = jnp.dot(attn, wo_v[:, cols], preferred_element_type=F32)
        proj[:, :, cols] = prod.reshape(ny, SUBROWS, TILE)

    def proj_piece(t, h):
        return proj.at[t, :, pl.ds(h * (half // 2), half // 2)]

    reduce_all(proj_piece, proj_in, on_ring_y, add_into)
    x_mid = (x_ref[ix * ny + iy, :, my_cols].astype(F32) + proj[iy]).astype(BF16).astype(F32)

    square = jnp.sum(x_mid * x_mid, axis=-1, keepdims=True)
    stat_out[...] = jnp.broadcast_to(square, stat_out.shape)
    swap = send(stat_out, stat_in, partner)
    swap.wait_recv()
    inv_rms = lax.rsqrt((stat_out[:, :1] + stat_in[:, :1]) / dim + NORM_EPS)
    gathered[core, ix, iy] = (x_mid * inv_rms * gain_ref[1:2, my_cols]).astype(BF16).astype(F32)

    quarter, eighth = half // 2, half // 4

    def portion(buf, lo, x_first):
        def cell(first, second, h=None):
            cols = pl.ds(lo, quarter) if h is None else pl.ds(lo + h * eighth, eighth)
            at = (first, second) if x_first else (second, first)
            return buf.at[(*at, slice(None), cols)]

        return cell, (on_ring_x, on_ring_y) if x_first else (on_ring_y, on_ring_x)

    def gather_all(buf):
        forwards = []

        def forward(ref):
            forwards.append(send(ref, ref, partner))

        forward(buf.at[core, ix, iy])

        def flow(lo, x_first):
            cell, (first, second) = portion(buf.at[core], lo, x_first)
            (f_at, f_right, f_left), (s_at, s_right, s_left) = first, second
            me = s_at(0)

            def both_ways(ref, right, left):
                return send(ref, ref, right), send(ref, ref, left)

            def pass_on(copies, from_l, from_r, right, left):
                copies[0].wait_recv()
                r = send(from_l(0), from_l(0), right)
                copies[1].wait_recv()
                return r, send(from_r(1), from_r(1), left)

            def second_start(t):
                return both_ways(cell(t, me), s_right, s_left)

            def second_turn(t, copies):
                far = pass_on(copies, lambda h: cell(t, s_at(-1), h), lambda h: cell(t, s_at(1), h), s_right, s_left)
                forward(cell(t, s_at(-1)))
                forward(cell(t, s_at(1)))
                return far

            def second_end(t, copies):
                for copy in copies:
                    copy.wait_recv()
                forward(cell(t, s_at(2)))

            near = both_ways(cell(f_at(0), me), f_right, f_left)
            own = second_start(f_at(0))
            yield
            far = pass_on(near, lambda h: cell(f_at(-1), me, h), lambda h: cell(f_at(1), me, h), f_right, f_left)
            from_l, from_r = second_start(f_at(-1)), second_start(f_at(1))
            forward(cell(f_at(-1), me))
            forward(cell(f_at(1), me))
            yield
            own = second_turn(f_at(0), own)
            yield
            for copy in far:
                copy.wait_recv()
            from_far = second_start(f_at(2))
            forward(cell(f_at(2), me))
            yield
            from_l, from_r = second_turn(f_at(-1), from_l), second_turn(f_at(1), from_r)
            yield
            second_end(f_at(0), own)
            yield
            from_far = second_turn(f_at(2), from_far)
            yield
            second_end(f_at(-1), from_l)
            second_end(f_at(1), from_r)
            yield
            second_end(f_at(2), from_far)

        run_together(flow(0, False), flow(quarter, True))
        for copy in forwards:
            copy.wait_recv()

    gather_all(gathered)
    rows = nx * ny * SUBROWS
    for c in range(CORES):
        normed[:, c * half : (c + 1) * half] = gathered[c].reshape(rows, half).astype(BF16)

    w1_load.wait()
    w3_load.wait()
    inner = w1_v.shape[1]
    step = 256
    acts = []
    for j in range(inner // step):
        cols = slice(j * step, (j + 1) * step)
        gate = jnp.dot(normed[...], w1_v[:, cols], preferred_element_type=F32)
        up = jnp.dot(normed[...], w3_v[:, cols], preferred_element_type=F32)
        acts.append((gate * jax.nn.sigmoid(gate) * up).astype(BF16))
    act = jnp.concatenate(acts, axis=-1)
    w2_load.wait()

    def down(which, j):
        cols = pl.ds(pl.multiple_of(which * half + j * TILE, TILE), TILE)
        return jnp.dot(act, w2_v[:, cols], preferred_element_type=F32).reshape(nx, ny, SUBROWS, TILE)

    swaps = []
    for j in range(tiles):
        cols = slice(j * TILE, (j + 1) * TILE)
        other[:, :, :, cols] = down(1 - core, j)
        swaps.append(send(other.at[:, :, :, cols], other_in.at[:, :, :, cols], partner))

    def reduce_flow(index):
        for j in range(index * tiles // 2, (index + 1) * tiles // 2):
            cols = slice(j * TILE, (j + 1) * TILE)
            swaps[j].wait_recv()
            mine[:, :, :, cols] = down(core, j) + other_in[:, :, :, cols]
        cell, (first, second) = portion(mine, index * quarter, index == 0)
        here, there = first[0](0), second[0]

        def begin(k, t):
            return reduce_begin(lambda to, h: cell(to, t, h), big_in.at[index, k], first, add_into)

        order = (there(2), there(1), there(-1), there(0))
        states = [begin(k, order[k]) for k in range(2)]
        yield
        reduce_turn(states[0])
        states.append(begin(2, order[2]))
        yield
        reduce_turn(states[1])
        states.append(begin(3, order[3]))
        yield
        reduce_turn(states[2])
        reduce_end(states[0])
        held = small_in.at[index]
        _, right, left = second

        def piece(t, h):
            return cell(here, t, h)

        r1 = send(piece(there(2), 0), held.at[0], right)
        l1 = send(piece(there(2), 1), held.at[1], left)
        yield
        reduce_turn(states[3])
        reduce_end(states[1])
        r2 = send(piece(there(1), 1), held.at[2], right)
        reduce_end(states[2])
        l2 = send(piece(there(-1), 0), held.at[3], left)
        yield
        last = [piece, held, second, add_into, r1, l1, r2, l2]
        reduce_turn(last)
        yield
        reduce_end(states[3])
        reduce_end(last)

    run_together(reduce_flow(0), reduce_flow(1))
    final[core, ix, iy] = (x_mid + mine[ix, iy]).astype(BF16).astype(F32)
    gather_all(final)
    for c in range(CORES):
        out_ref[:, c * half : (c + 1) * half] = final[c].reshape(rows, half).astype(BF16)
    for copy in sent:
        copy.wait_send()


def front_kernel(
    group_size, kv_local,
    x_ref, gain_ref, cos_ref, sin_ref, pos_ref, wq_hbm, wk_hbm, wv_hbm, k_hbm, v_hbm,
    parts_ref, k_out_hbm, v_out_hbm, k_new_ref, v_new_ref,
    wq_v, wk_v, wv_v, k_buf, v_buf, normed, q_rows, num_rows, max_rows, sum_rows, k_rows, v_rows,
    load_sem, store_sem,
):
    rows, dim = x_ref.shape
    columns = k_buf.shape[1]
    block_len = columns // kv_local
    head_dim = k_buf.shape[2]
    slots = SUBROWS * kv_local
    first_slot = lax.axis_index("sp") * block_len
    scale = head_dim ** -0.5

    loads = []

    def load(src, dst):
        copy = pltpu.make_async_copy(src, dst, load_sem.at[len(loads)])
        copy.start()
        loads.append(copy)
        return copy

    step = 2 * head_dim
    q_steps = wq_v.shape[1] // step
    early = q_steps // 2
    wk_load = load(wk_hbm, wk_v)
    wv_load = load(wv_hbm, wv_v)
    q_loads = [load(wq_hbm.at[:, pl.ds(j * step, step)], wq_v.at[:, pl.ds(j * step, step)]) for j in range(early)]
    k_load = load(k_hbm, k_buf)
    v_load = load(v_hbm, v_buf)
    q_loads += [load(wq_hbm.at[:, pl.ds(j * step, step)], wq_v.at[:, pl.ds(j * step, step)]) for j in range(early, q_steps)]

    q_rows[...] = jnp.zeros_like(q_rows)
    block = 2 * SUBROWS

    @pl.loop(0, rows // block)
    def _(i):
        at = pl.ds(pl.multiple_of(i * block, block), block)
        vals = x_ref[at, :].astype(F32)
        inv_rms = lax.rsqrt(jnp.mean(vals * vals, axis=-1, keepdims=True) + NORM_EPS)
        normed[at, :] = (vals * inv_rms * gain_ref[:1, :]).astype(BF16)

    def rotate(vals):
        vals = vals.astype(BF16).astype(F32)
        return (vals * cos_ref[...] + pltpu.roll(vals, head_dim // 2, 1) * sin_ref[...]).astype(BF16)

    wk_load.wait()
    k_proj = jnp.dot(normed[...], wk_v[...], preferred_element_type=F32)
    for k in range(kv_local):
        cols = slice(k * head_dim, (k + 1) * head_dim)
        k_rows[pl.ds(k, rows, stride=kv_local), :] = rotate(k_proj[:, cols]).astype(F32)
    k_new_ref[...] = k_rows[...].astype(BF16)
    wv_load.wait()
    v_proj = jnp.dot(normed[...], wv_v[...], preferred_element_type=F32).astype(BF16)
    for k in range(kv_local):
        v_rows[pl.ds(k, rows, stride=kv_local), :] = v_proj[:, k * head_dim : (k + 1) * head_dim].astype(F32)
    v_new_ref[...] = v_rows[...].astype(BF16)

    def project(j):
        q_loads[j].wait()
        prod = jnp.dot(normed[...], wq_v[:, j * step : (j + 1) * step], preferred_element_type=F32)
        for n in range(step // head_dim):
            head = j * (step // head_dim) + n
            row = head // group_size * SUBROWS + head % group_size
            q_rows[pl.ds(row, rows, stride=slots), :] = rotate(prod[:, n * head_dim : (n + 1) * head_dim]).astype(F32)

    for j in range(early + 1):
        project(j)
    k_load.wait()
    v_load.wait()
    sub = lax.broadcasted_iota(jnp.int32, (block, head_dim), 0)
    per_block = block // kv_local

    @pl.loop(0, rows)
    def _(b):
        p = pos_ref[b] - first_slot

        @pl.when((p >= 0) & (p < block_len))
        def _():
            at = pl.ds(pl.multiple_of(p // per_block * block, block), block)
            hit = sub // kv_local == p % per_block
            for buf, new_rows in ((k_buf, k_rows), (v_buf, v_rows)):
                new = new_rows[pl.ds(b * kv_local, 1), :]
                for k in range(1, kv_local):
                    new = jnp.where(sub % kv_local == k, new_rows[pl.ds(b * kv_local + k, 1), :], new)
                buf[b, at, :] = jnp.where(hit, new, buf[b, at, :].astype(F32)).astype(BF16)

    for j in range(early + 1, q_steps):
        project(j)
    stores = [
        pltpu.make_async_copy(k_buf, k_out_hbm, store_sem.at[0]),
        pltpu.make_async_copy(v_buf, v_out_hbm, store_sem.at[1]),
    ]
    for store in stores:
        store.start()

    col = lax.broadcasted_iota(jnp.int32, (slots, columns), 1)
    own_head = col % kv_local == lax.broadcasted_iota(jnp.int32, (slots, columns), 0) // SUBROWS
    time = jnp.where(own_head, first_slot + col // kv_local, jnp.iinfo(jnp.int32).max)
    together = 16

    @pl.loop(0, rows // together)
    def _(i):
        group = [i * together + u for u in range(together)]
        spans = [pl.ds(pl.multiple_of(b * slots, slots), slots) for b in group]
        scores = [
            lax.dot_general(q_rows[at, :].astype(BF16), k_buf[b], (((1,), (1,)), ((), ())), preferred_element_type=F32)
            for b, at in zip(group, spans)
        ]
        packed = []
        for b, at, score in zip(group, spans, scores):
            valid = time <= pos_ref[b]
            score = jnp.where(valid, score * scale, MASK_FILL)
            top = jnp.max(score, axis=-1, keepdims=True)
            weights = jnp.where(valid, jnp.exp(score - top), 0.0)
            total = jnp.sum(weights, axis=-1, keepdims=True)
            max_rows[at, :] = jnp.broadcast_to(top, (slots, LANES))
            sum_rows[at, :] = jnp.broadcast_to(total, (slots, LANES))
            packed.append(weights.astype(BF16))
        nums = [jnp.dot(w, v_buf[b], preferred_element_type=F32) for b, w in zip(group, packed)]
        for at, num in zip(spans, nums):
            num_rows[at, :] = num

    lane = lax.broadcasted_iota(jnp.int32, (rows, LANES), 1)
    width = group_size * head_dim
    for k in range(kv_local):
        stats = jnp.zeros((rows, LANES), F32)
        for g in range(group_size):
            at = pl.ds(k * SUBROWS + g, rows, stride=slots)
            parts_ref[k, :, g * head_dim : (g + 1) * head_dim] = num_rows[at, :]
            stats = jnp.where(lane == g, max_rows[at, :], stats)
            stats = jnp.where(lane == LANES // 2 + g, sum_rows[at, :], stats)
        parts_ref[k, :, width:] = stats
    for store in stores:
        store.wait()


def front_of_layer(x_in, gain, cos_part, sin_part, positions, w_q, w_k, w_v, k_flat, v_flat, kv_local):
    rows, dim = x_in.shape
    columns, head_dim = k_flat.shape[1:]
    group_size = w_q.shape[1] // head_dim // kv_local
    assert group_size <= SUBROWS
    slots = SUBROWS * kv_local
    hbm_spec = pl.BlockSpec(memory_space=pltpu.HBM)
    vmem_spec = pl.BlockSpec(memory_space=pltpu.VMEM)
    smem_spec = pl.BlockSpec(memory_space=pltpu.SMEM)
    row_buf = pltpu.VMEM((rows * slots, LANES), F32)
    new_buf = pltpu.VMEM((rows * kv_local, head_dim), F32)
    return pl.pallas_call(
        functools.partial(front_kernel, group_size, kv_local),
        out_shape=(
            jax.ShapeDtypeStruct((kv_local, rows, group_size * head_dim + LANES), F32),
            jax.ShapeDtypeStruct(k_flat.shape, BF16),
            jax.ShapeDtypeStruct(v_flat.shape, BF16),
            jax.ShapeDtypeStruct((rows * kv_local, head_dim), BF16),
            jax.ShapeDtypeStruct((rows * kv_local, head_dim), BF16),
        ),
        in_specs=[vmem_spec] * 4 + [smem_spec] + [hbm_spec] * 5,
        out_specs=(vmem_spec, hbm_spec, hbm_spec, vmem_spec, vmem_spec),
        scratch_shapes=[
            pltpu.VMEM(w_q.shape, BF16),
            pltpu.VMEM(w_k.shape, BF16),
            pltpu.VMEM(w_v.shape, BF16),
            pltpu.VMEM(k_flat.shape, BF16),
            pltpu.VMEM(v_flat.shape, BF16),
            pltpu.VMEM(x_in.shape, BF16),
            row_buf, row_buf, row_buf, row_buf, new_buf, new_buf,
            pltpu.SemaphoreType.DMA((w_q.shape[1] // (2 * head_dim) + 4,)),
            pltpu.SemaphoreType.DMA((2,)),
        ],
        compiler_params=pltpu.CompilerParams(vmem_limit_bytes=60 * 1024 * 1024),
        name="front_of_layer",
    )(x_in, gain, cos_part, sin_part, positions, w_q, w_k, w_v, k_flat, v_flat)


def rest_of_layer(mesh, parts, own_x, gains, w_o, w_gate, w_up, w_down):
    nx, ny = mesh.shape["sp"] // CORES, mesh.shape["tp"]
    dim = w_o.shape[1]
    half = dim // CORES
    rows = nx * ny * SUBROWS
    heads_width = parts.shape[-1] - LANES
    eighth = half // 4
    any_spec = pl.BlockSpec(memory_space=pltpu.HBM)
    vmem_spec = pl.BlockSpec(memory_space=pltpu.VMEM)
    width = heads_width + LANES
    chunk_rows = ny * SUBROWS
    count = 226
    scratch = [
        pltpu.VMEM((w_o.shape[0], half), BF16),
        pltpu.VMEM(w_gate.shape, BF16),
        pltpu.VMEM(w_up.shape, BF16),
        pltpu.VMEM(w_down.shape, BF16),
        pltpu.SemaphoreType.DMA((4,)),
        pltpu.VMEM((nx, chunk_rows, width), F32),
        pltpu.VMEM((nx, chunk_rows, width), F32),
        pltpu.VMEM((6, chunk_rows // 2, width), F32),
        pltpu.VMEM((CORES, chunk_rows, heads_width), F32),
        pltpu.VMEM((ny, SUBROWS, half), F32),
        pltpu.VMEM((6, SUBROWS, half // 2), F32),
        pltpu.VMEM((SUBROWS, LANES), F32),
        pltpu.VMEM((SUBROWS, LANES), F32),
        pltpu.VMEM((CORES, nx, ny, SUBROWS, half), F32),
        pltpu.VMEM((rows, dim), BF16),
        pltpu.VMEM((nx, ny, SUBROWS, half), F32),
        pltpu.VMEM((nx, ny, SUBROWS, half), F32),
        pltpu.VMEM((nx, ny, SUBROWS, half), F32),
        pltpu.VMEM((2, nx, 6, SUBROWS, eighth), F32),
        pltpu.VMEM((2, 6, SUBROWS, eighth), F32),
        pltpu.VMEM((CORES, nx, ny, SUBROWS, half), F32),
        pltpu.SemaphoreType.DMA((count,)),
        pltpu.SemaphoreType.DMA((count,)),
    ]
    return pl.pallas_call(
        functools.partial(rest_kernel, nx, ny, dim),
        out_shape=jax.ShapeDtypeStruct((rows, dim), BF16),
        in_specs=[vmem_spec] * 3 + [any_spec] * 4,
        out_specs=vmem_spec,
        scratch_shapes=scratch,
        compiler_params=pltpu.CompilerParams(collective_id=0, has_side_effects=True, vmem_limit_bytes=50 * 1024 * 1024),
        name="rest_of_layer",
    )(parts, gains, own_x, w_o, w_gate, w_up, w_down)


def solution(mesh):
    row_spec = P('dp', None)
    cache_spec = P('dp', 'sp', 'tp', None)
    new_spec = P('dp', 'tp', None)
    in_specs = (row_spec, P('dp'), cache_spec, cache_spec, P(None), P(None, 'tp'), P(None, 'tp'), P(None, 'tp'), P('tp', None), P(None), P(None, ('tp', 'sp')), P(None, ('tp', 'sp')), P(('tp', 'sp'), None))
    out_specs = (row_spec, cache_spec, cache_spec, new_spec, new_spec)
    nx, ny = mesh.shape["sp"] // CORES, mesh.shape["tp"]

    def local_step(x_in, positions, k_cache, v_cache, attn_gain, w_q, w_k, w_v, w_o, mlp_gain, w_gate, w_up, w_down):
        num_rows, block_len, kv_local, head_dim = k_cache.shape
        dim = x_in.shape[1]
        gains = jnp.stack([attn_gain, mlp_gain]).astype(F32)
        cos_part, sin_part = rotary_tables(positions, head_dim)
        flat = (num_rows, block_len * kv_local, head_dim)
        parts, k_out, v_out, k_new, v_new = front_of_layer(
            x_in, gains, cos_part, sin_part, positions, w_q, w_k, w_v,
            k_cache.reshape(flat), v_cache.reshape(flat), kv_local,
        )
        k_out, v_out = k_out.reshape(k_cache.shape), v_out.reshape(v_cache.shape)
        k_new, v_new = k_new.reshape(num_rows, kv_local, head_dim), v_new.reshape(num_rows, kv_local, head_dim)
        parts = parts.reshape(kv_local, nx, num_rows // nx, parts.shape[-1])
        own_x = x_in.reshape(nx * ny, SUBROWS, dim)
        x_out = rest_of_layer(mesh, parts, own_x, gains, w_o, w_gate, w_up, w_down)
        return x_out, k_out, v_out, k_new, v_new

    return jax.shard_map(local_step, mesh=mesh, in_specs=in_specs, out_specs=out_specs, check_vma=False)
```

```python
import functools

import jax
import jax.numpy as jnp
from jax import lax
from jax.experimental import pallas as pl
from jax.experimental.pallas import tpu as pltpu
from jax.sharding import PartitionSpec as P

ROPE_THETA = 1000000.0
NORM_EPS = 1e-05
MASK_FILL = -1.0e30
LANES = 128
SUBROWS = 8
CORES = 2
TILE = 512
MESH = pl.DeviceIdType.MESH
F32 = jnp.float32
BF16 = jnp.bfloat16


def rotary_tables(positions, head_dim):
    half_dim = head_dim // 2
    inv_freq = ROPE_THETA ** (jnp.arange(half_dim, dtype=F32) * (-2.0 / head_dim))
    angles = positions.astype(F32)[:, None] * inv_freq[None, :]
    cos_part, sin_part = jnp.cos(angles), jnp.sin(angles)
    return cos_part, sin_part


def run_together(*flows):
    flows = list(flows)
    while flows:
        for flow in list(flows):
            if next(flow, flow) is flow:
                flows.remove(flow)


def merge_partials(left, right):
    width = left.shape[-1] - LANES
    stat_l, stat_r = left[:, width:], right[:, width:]
    lane = lax.broadcasted_iota(jnp.int32, stat_l.shape, 1)
    top = jnp.maximum(stat_l, stat_r)
    scale_l, scale_r = jnp.exp(stat_l - top), jnp.exp(stat_r - top)
    total = stat_l * pltpu.roll(scale_l, LANES // 2, 1) + stat_r * pltpu.roll(scale_r, LANES // 2, 1)
    parts = []
    for g in range(width // LANES):
        cols = slice(g * LANES, (g + 1) * LANES)
        parts.append(left[:, cols] * scale_l[:, g : g + 1] + right[:, cols] * scale_r[:, g : g + 1])
    parts.append(jnp.where(lane < LANES // 2, top, total))
    return jnp.concatenate(parts, axis=-1)


def rest_kernel(
    nx, ny, dim,
    part_ref, gain_ref, x_ref, wo_hbm, w1_hbm, w3_hbm, w2_hbm,
    out_ref,
    wo_v, w1_v, w3_v, w2_v, load_sem,
    pair_in, ring_a, ring_a_in, o_in, proj, proj_in, stat_out, stat_in,
    gathered, normed, other, other_in, mine, big_in, small_in, final,
    send_sem, recv_sem,
):
    sp, iy = lax.axis_index("sp"), lax.axis_index("tp")
    ix, core = sp // CORES, lax.rem(sp, CORES)
    half = wo_v.shape[1]
    heads_width = part_ref.shape[-1] - LANES

    def on_x(step):
        return lax.rem(ix + step + nx, nx)

    def on_y(step):
        return lax.rem(iy + step + ny, ny)

    partner = {"sp": ix * CORES + (1 - core)}
    x_right, x_left = {"sp": on_x(1) * CORES + core}, {"sp": on_x(-1) * CORES + core}
    y_right, y_left = {"tp": on_y(1)}, {"tp": on_y(-1)}

    loads = []

    def load(src, dst):
        copy = pltpu.make_async_copy(src, dst, load_sem.at[len(loads)])
        copy.start()
        loads.append(copy)
        return copy

    my_cols = pl.ds(pl.multiple_of(core * half, half), half)
    wo_load = load(wo_hbm.at[:, my_cols], wo_v)
    w1_load = load(w1_hbm, w1_v)
    w3_load = load(w3_hbm, w3_v)
    w2_load = load(w2_hbm, w2_v)

    barrier = pltpu.get_barrier_semaphore()
    peers = (partner, x_right, x_left, y_right, y_left)
    for peer in peers:
        pl.semaphore_signal(barrier, inc=1, device_id=peer, device_id_type=MESH)
    pl.semaphore_wait(barrier, len(peers))

    sent = []

    def send(src, dst, peer):
        k = len(sent)
        copy = pltpu.make_async_remote_copy(
            src_ref=src, dst_ref=dst, send_sem=send_sem.at[k], recv_sem=recv_sem.at[k], device_id=peer, device_id_type=MESH
        )
        copy.start()
        sent.append(copy)
        return copy

    on_ring_x, on_ring_y = (on_x, x_right, x_left), (on_y, y_right, y_left)

    def reduce_begin(piece, held, ring, add):
        at, right, left = ring
        r1 = send(piece(at(2), 0), held.at[0], right)
        l1 = send(piece(at(2), 1), held.at[1], left)
        r2 = send(piece(at(1), 1), held.at[2], right)
        l2 = send(piece(at(-1), 0), held.at[3], left)
        return [piece, held, ring, add, r1, l1, r2, l2]

    def reduce_turn(state):
        piece, held, (at, right, left), add, r1, l1 = state[:6]
        r1.wait_recv()
        add(piece(at(1), 0), held.at[0])
        state.append(send(piece(at(1), 0), held.at[4], right))
        l1.wait_recv()
        add(piece(at(-1), 1), held.at[1])
        state.append(send(piece(at(-1), 1), held.at[5], left))

    def reduce_end(state):
        piece, held, (at, _, _), add, _, _, r2, l2, r3, l3 = state
        for copy, h, k in ((l2, 0, 3), (r2, 1, 2), (r3, 0, 4), (l3, 1, 5)):
            copy.wait_recv()
            add(piece(at(0), h), held.at[k])

    def reduce_all(piece, held, ring, add):
        state = reduce_begin(piece, held, ring, add)
        reduce_turn(state)
        reduce_end(state)

    def add_into(dst, src):
        dst[...] = dst[...] + src[...]

    order = (on_x(2), on_x(1), on_x(-1), on_x(0))
    swaps = [send(part_ref.at[1 - core, t], pair_in.at[t], partner) for t in order]
    for t, swap in zip(order, swaps):
        swap.wait_recv()
        ring_a[t] = merge_partials(part_ref[core, t], pair_in[t])

    rows_half = ring_a.shape[1] // 2

    def part_piece(t, h):
        return ring_a.at[t, pl.ds(h * rows_half, rows_half)]

    def merge_into(dst, src):
        dst[...] = merge_partials(dst[...], src[...])

    reduce_all(part_piece, ring_a_in, on_ring_x, merge_into)
    merged = ring_a[on_x(0)]
    stats = merged[:, heads_width:]
    heads = []
    for g in range(heads_width // LANES):
        lsum = stats[:, LANES // 2 + g : LANES // 2 + g + 1]
        heads.append(merged[:, g * LANES : (g + 1) * LANES] / lsum)
    o_in[core] = jnp.concatenate(heads, axis=-1).astype(BF16).astype(F32)
    swap = send(o_in.at[core], o_in.at[core], partner)
    swap.wait_recv()
    attn = jnp.concatenate([o_in[c] for c in range(CORES)], axis=-1).astype(BF16)

    wo_load.wait()
    tiles = half // TILE
    for j in range(tiles):
        cols = slice(j * TILE, (j + 1) * TILE)
        prod = jnp.dot(attn, wo_v[:, cols], preferred_element_type=F32)
        proj[:, :, cols] = prod.reshape(ny, SUBROWS, TILE)

    def proj_piece(t, h):
        return proj.at[t, :, pl.ds(h * (half // 2), half // 2)]

    reduce_all(proj_piece, proj_in, on_ring_y, add_into)
    x_mid = (x_ref[...] + proj[iy]).astype(BF16).astype(F32)

    square = jnp.sum(x_mid * x_mid, axis=-1, keepdims=True)
    stat_out[...] = jnp.broadcast_to(square, stat_out.shape)
    swap = send(stat_out, stat_in, partner)
    swap.wait_recv()
    inv_rms = lax.rsqrt((stat_out[:, :1] + stat_in[:, :1]) / dim + NORM_EPS)
    gathered[core, ix, iy] = (x_mid * inv_rms * gain_ref[1:2, my_cols]).astype(BF16).astype(F32)

    quarter = half // 2

    def either(for_one, for_zero):
        return core * for_one + (1 - core) * for_zero

    def ring_of(step_x, step_y):
        def at(step):
            return step_x * on_x(step) + step_y * on_y(step)

        def peer(step):
            to_x = step_x * on_x(step) + (1 - step_x) * ix
            to_y = step_y * on_y(step) + (1 - step_y) * iy
            return {"sp": to_x * CORES + core, "tp": to_y}

        return at, peer(1), peer(-1)

    own_ring, other_ring = ring_of(core, 1 - core), ring_of(1 - core, core)

    def cells(buf, core_first):
        def cell(first, second, h=None):
            cols = slice(None) if h is None else pl.ds(h * quarter, quarter)
            a, b = (first, second) if core_first else (second, first)
            return buf.at[either(a, b), either(b, a), :, cols]

        return cell

    def gather_all(buf):
        forwards = []

        def forward(ref):
            forwards.append(send(ref, ref, partner))

        forward(buf.at[core, ix, iy])

        def flow():
            cell, first, second = cells(buf.at[core], True), own_ring, other_ring
            (f_at, f_right, f_left), (s_at, s_right, s_left) = first, second
            me = s_at(0)

            def both_ways(ref, right, left):
                return send(ref, ref, right), send(ref, ref, left)

            def pass_on(copies, from_l, from_r, right, left):
                copies[0].wait_recv()
                r = send(from_l(0), from_l(0), right)
                copies[1].wait_recv()
                return r, send(from_r(1), from_r(1), left)

            def second_start(t):
                return both_ways(cell(t, me), s_right, s_left)

            def second_turn(t, copies):
                far = pass_on(copies, lambda h: cell(t, s_at(-1), h), lambda h: cell(t, s_at(1), h), s_right, s_left)
                forward(cell(t, s_at(-1)))
                forward(cell(t, s_at(1)))
                return far

            def second_end(t, copies):
                for copy in copies:
                    copy.wait_recv()
                forward(cell(t, s_at(2)))

            near = both_ways(cell(f_at(0), me), f_right, f_left)
            own = second_start(f_at(0))
            yield
            far = pass_on(near, lambda h: cell(f_at(-1), me, h), lambda h: cell(f_at(1), me, h), f_right, f_left)
            from_l, from_r = second_start(f_at(-1)), second_start(f_at(1))
            forward(cell(f_at(-1), me))
            forward(cell(f_at(1), me))
            yield
            own = second_turn(f_at(0), own)
            yield
            for copy in far:
                copy.wait_recv()
            from_far = second_start(f_at(2))
            forward(cell(f_at(2), me))
            yield
            from_l, from_r = second_turn(f_at(-1), from_l), second_turn(f_at(1), from_r)
            yield
            second_end(f_at(0), own)
            yield
            from_far = second_turn(f_at(2), from_far)
            yield
            second_end(f_at(-1), from_l)
            second_end(f_at(1), from_r)
            yield
            second_end(f_at(2), from_far)

        run_together(flow())
        for copy in forwards:
            copy.wait_recv()

    gather_all(gathered)
    rows = nx * ny * SUBROWS
    for c in range(CORES):
        normed[:, c * half : (c + 1) * half] = gathered[c].reshape(rows, half).astype(BF16)

    w1_load.wait()
    w3_load.wait()
    inner = w1_v.shape[1]
    step = 256
    acts = []
    for j in range(inner // step):
        cols = slice(j * step, (j + 1) * step)
        gate = jnp.dot(normed[...], w1_v[:, cols], preferred_element_type=F32)
        up = jnp.dot(normed[...], w3_v[:, cols], preferred_element_type=F32)
        acts.append((gate * jax.nn.sigmoid(gate) * up).astype(BF16))
    act = jnp.concatenate(acts, axis=-1)
    w2_load.wait()

    def down(which, j):
        cols = pl.ds(pl.multiple_of(which * half + j * TILE, TILE), TILE)
        return jnp.dot(act, w2_v[:, cols], preferred_element_type=F32).reshape(nx, ny, SUBROWS, TILE)

    swaps = []
    for j in range(tiles):
        cols = slice(j * TILE, (j + 1) * TILE)
        other[:, :, :, cols] = down(1 - core, j)
        swaps.append(send(other.at[:, :, :, cols], other_in.at[:, :, :, cols], partner))

    def reduce_flow():
        for j in range(tiles):
            cols = slice(j * TILE, (j + 1) * TILE)
            swaps[j].wait_recv()
            mine[:, :, :, cols] = down(core, j) + other_in[:, :, :, cols]
        cell, first, second = cells(mine, False), other_ring, own_ring
        here, there = first[0](0), second[0]

        def begin(k, t):
            return reduce_begin(lambda to, h: cell(to, t, h), big_in.at[k], first, add_into)

        order = (there(2), there(1), there(-1), there(0))
        states = [begin(k, order[k]) for k in range(2)]
        yield
        reduce_turn(states[0])
        states.append(begin(2, order[2]))
        yield
        reduce_turn(states[1])
        states.append(begin(3, order[3]))
        yield
        reduce_turn(states[2])
        reduce_end(states[0])
        held = small_in
        _, right, left = second

        def piece(t, h):
            return cell(here, t, h)

        r1 = send(piece(there(2), 0), held.at[0], right)
        l1 = send(piece(there(2), 1), held.at[1], left)
        yield
        reduce_turn(states[3])
        reduce_end(states[1])
        r2 = send(piece(there(1), 1), held.at[2], right)
        reduce_end(states[2])
        l2 = send(piece(there(-1), 0), held.at[3], left)
        yield
        last = [piece, held, second, add_into, r1, l1, r2, l2]
        reduce_turn(last)
        yield
        reduce_end(states[3])
        reduce_end(last)

    run_together(reduce_flow())
    final[core, ix, iy] = (x_mid + mine[ix, iy]).astype(BF16).astype(F32)
    gather_all(final)
    for c in range(CORES):
        out_ref[:, c * half : (c + 1) * half] = final[c].reshape(rows, half).astype(BF16)
    for copy in sent:
        copy.wait_send()


def front_kernel(
    group_size, kv_local, ny,
    x_ref, gain_ref, cos_ref, sin_ref, pos_ref, wq_hbm, wk_hbm, wv_hbm, k_hbm, v_hbm,
    parts_ref, k_out_hbm, v_out_hbm, k_new_ref, v_new_ref, own_x_ref,
    wq_v, wk_v, wv_v, k_buf, v_buf, normed, q_rows, num_rows, max_rows, sum_rows, k_rows, v_rows, cos_all, sin_all,
    load_sem, store_sem,
):
    rows, dim = normed.shape
    sp = lax.axis_index("sp")
    own_cols = pl.ds(pl.multiple_of(lax.rem(sp, CORES) * (dim // CORES), dim // CORES), dim // CORES)
    own_x_ref[...] = x_ref[sp // CORES * ny + lax.axis_index("tp"), :, own_cols].astype(F32)
    columns = k_buf.shape[1]
    block_len = columns // kv_local
    head_dim = k_buf.shape[2]
    slots = SUBROWS * kv_local
    first_slot = lax.axis_index("sp") * block_len
    scale = head_dim ** -0.5

    loads = []

    def load(src, dst):
        copy = pltpu.make_async_copy(src, dst, load_sem.at[len(loads)])
        copy.start()
        loads.append(copy)
        return copy

    step = 2 * head_dim
    q_steps = wq_v.shape[1] // step
    early = q_steps // 2
    wk_load = load(wk_hbm, wk_v)
    wv_load = load(wv_hbm, wv_v)
    q_loads = [load(wq_hbm.at[:, pl.ds(j * step, step)], wq_v.at[:, pl.ds(j * step, step)]) for j in range(early)]
    k_load = load(k_hbm, k_buf)
    v_load = load(v_hbm, v_buf)
    q_loads += [load(wq_hbm.at[:, pl.ds(j * step, step)], wq_v.at[:, pl.ds(j * step, step)]) for j in range(early, q_steps)]

    q_rows[...] = jnp.zeros_like(q_rows)
    block = 2 * SUBROWS

    @pl.loop(0, rows // block)
    def _(i):
        at = pl.ds(pl.multiple_of(i * block, block), block)
        vals = x_ref[pl.ds(i * (block // SUBROWS), block // SUBROWS)].astype(F32).reshape(block, dim)
        inv_rms = lax.rsqrt(jnp.mean(vals * vals, axis=-1, keepdims=True) + NORM_EPS)
        normed[at, :] = (vals * inv_rms * gain_ref[:1, :]).astype(BF16)

    cos_all[...] = jnp.concatenate([cos_ref[...], cos_ref[...]], axis=-1)
    sin_all[...] = jnp.concatenate([-sin_ref[...], sin_ref[...]], axis=-1)

    def rotate(vals):
        vals = vals.astype(BF16).astype(F32)
        return (vals * cos_all[...] + pltpu.roll(vals, head_dim // 2, 1) * sin_all[...]).astype(BF16)

    wk_load.wait()
    k_proj = jnp.dot(normed[...], wk_v[...], preferred_element_type=F32)
    for k in range(kv_local):
        cols = slice(k * head_dim, (k + 1) * head_dim)
        k_rows[pl.ds(k, rows, stride=kv_local), :] = rotate(k_proj[:, cols]).astype(F32)
    k_new_ref[...] = k_rows[...].astype(BF16)
    wv_load.wait()
    v_proj = jnp.dot(normed[...], wv_v[...], preferred_element_type=F32).astype(BF16)
    for k in range(kv_local):
        v_rows[pl.ds(k, rows, stride=kv_local), :] = v_proj[:, k * head_dim : (k + 1) * head_dim].astype(F32)
    v_new_ref[...] = v_rows[...].astype(BF16)

    def project(j):
        q_loads[j].wait()
        prod = jnp.dot(normed[...], wq_v[:, j * step : (j + 1) * step], preferred_element_type=F32)
        for n in range(step // head_dim):
            head = j * (step // head_dim) + n
            row = head // group_size * SUBROWS + head % group_size
            q_rows[pl.ds(row, rows, stride=slots), :] = rotate(prod[:, n * head_dim : (n + 1) * head_dim]).astype(F32)

    for j in range(early + 1):
        project(j)
    k_load.wait()
    v_load.wait()
    sub = lax.broadcasted_iota(jnp.int32, (block, head_dim), 0)
    per_block = block // kv_local

    @pl.loop(0, rows)
    def _(b):
        p = pos_ref[b] - first_slot

        @pl.when((p >= 0) & (p < block_len))
        def _():
            at = pl.ds(pl.multiple_of(p // per_block * block, block), block)
            hit = sub // kv_local == p % per_block
            for buf, new_rows in ((k_buf, k_rows), (v_buf, v_rows)):
                new = new_rows[pl.ds(b * kv_local, 1), :]
                for k in range(1, kv_local):
                    new = jnp.where(sub % kv_local == k, new_rows[pl.ds(b * kv_local + k, 1), :], new)
                buf[b, at, :] = jnp.where(hit, new, buf[b, at, :].astype(F32)).astype(BF16)

    for j in range(early + 1, q_steps):
        project(j)
    stores = [
        pltpu.make_async_copy(k_buf, k_out_hbm, store_sem.at[0]),
        pltpu.make_async_copy(v_buf, v_out_hbm, store_sem.at[1]),
    ]
    for store in stores:
        store.start()

    col = lax.broadcasted_iota(jnp.int32, (slots, columns), 1)
    own_head = col % kv_local == lax.broadcasted_iota(jnp.int32, (slots, columns), 0) // SUBROWS
    time = jnp.where(own_head, first_slot + col // kv_local, jnp.iinfo(jnp.int32).max)
    together = 16

    @pl.loop(0, rows // together)
    def _(i):
        group = [i * together + u for u in range(together)]
        spans = [pl.ds(pl.multiple_of(b * slots, slots), slots) for b in group]
        scores = [
            lax.dot_general(q_rows[at, :].astype(BF16), k_buf[b], (((1,), (1,)), ((), ())), preferred_element_type=F32)
            for b, at in zip(group, spans)
        ]
        packed = []
        for b, at, score in zip(group, spans, scores):
            valid = time <= pos_ref[b]
            score = jnp.where(valid, score * scale, MASK_FILL)
            top = jnp.max(score, axis=-1, keepdims=True)
            weights = jnp.where(valid, jnp.exp(score - top), 0.0)
            total = jnp.sum(weights, axis=-1, keepdims=True)
            max_rows[at, :] = jnp.broadcast_to(top, (slots, LANES))
            sum_rows[at, :] = jnp.broadcast_to(total, (slots, LANES))
            packed.append(weights.astype(BF16))
        nums = [jnp.dot(w, v_buf[b], preferred_element_type=F32) for b, w in zip(group, packed)]
        for at, num in zip(spans, nums):
            num_rows[at, :] = num

    lane = lax.broadcasted_iota(jnp.int32, (rows, LANES), 1)
    width = group_size * head_dim
    for k in range(kv_local):
        stats = jnp.zeros((rows, LANES), F32)
        for g in range(group_size):
            at = pl.ds(k * SUBROWS + g, rows, stride=slots)
            parts_ref[k, :, g * head_dim : (g + 1) * head_dim] = num_rows[at, :]
            stats = jnp.where(lane == g, max_rows[at, :], stats)
            stats = jnp.where(lane == LANES // 2 + g, sum_rows[at, :], stats)
        parts_ref[k, :, width:] = stats
    for store in stores:
        store.wait()


def front_of_layer(x_in, gain, cos_part, sin_part, positions, w_q, w_k, w_v, k_flat, v_flat, kv_local, ny):
    rows, dim = x_in.shape[0] * x_in.shape[1], x_in.shape[2]
    columns, head_dim = k_flat.shape[1:]
    group_size = w_q.shape[1] // head_dim // kv_local
    assert group_size <= SUBROWS
    slots = SUBROWS * kv_local
    hbm_spec = pl.BlockSpec(memory_space=pltpu.HBM)
    vmem_spec = pl.BlockSpec(memory_space=pltpu.VMEM)
    smem_spec = pl.BlockSpec(memory_space=pltpu.SMEM)
    row_buf = pltpu.VMEM((rows * slots, LANES), F32)
    new_buf = pltpu.VMEM((rows * kv_local, head_dim), F32)
    return pl.pallas_call(
        functools.partial(front_kernel, group_size, kv_local, ny),
        out_shape=(
            jax.ShapeDtypeStruct((kv_local, rows, group_size * head_dim + LANES), F32),
            jax.ShapeDtypeStruct(k_flat.shape, BF16),
            jax.ShapeDtypeStruct(v_flat.shape, BF16),
            jax.ShapeDtypeStruct((rows * kv_local, head_dim), BF16),
            jax.ShapeDtypeStruct((rows * kv_local, head_dim), BF16),
            jax.ShapeDtypeStruct((SUBROWS, dim // CORES), F32),
        ),
        in_specs=[vmem_spec] * 4 + [smem_spec] + [hbm_spec] * 5,
        out_specs=(vmem_spec, hbm_spec, hbm_spec, vmem_spec, vmem_spec, vmem_spec),
        scratch_shapes=[
            pltpu.VMEM(w_q.shape, BF16),
            pltpu.VMEM(w_k.shape, BF16),
            pltpu.VMEM(w_v.shape, BF16),
            pltpu.VMEM(k_flat.shape, BF16),
            pltpu.VMEM(v_flat.shape, BF16),
            pltpu.VMEM((rows, dim), BF16),
            row_buf, row_buf, row_buf, row_buf, new_buf, new_buf,
            pltpu.VMEM((rows, head_dim), F32),
            pltpu.VMEM((rows, head_dim), F32),
            pltpu.SemaphoreType.DMA((w_q.shape[1] // (2 * head_dim) + 4,)),
            pltpu.SemaphoreType.DMA((2,)),
        ],
        compiler_params=pltpu.CompilerParams(vmem_limit_bytes=60 * 1024 * 1024),
        name="front_of_layer",
    )(x_in, gain, cos_part, sin_part, positions, w_q, w_k, w_v, k_flat, v_flat)


def rest_of_layer(mesh, parts, own_x, gains, w_o, w_gate, w_up, w_down):
    nx, ny = mesh.shape["sp"] // CORES, mesh.shape["tp"]
    dim = w_o.shape[1]
    half = dim // CORES
    rows = nx * ny * SUBROWS
    heads_width = parts.shape[-1] - LANES
    any_spec = pl.BlockSpec(memory_space=pltpu.HBM)
    vmem_spec = pl.BlockSpec(memory_space=pltpu.VMEM)
    width = heads_width + LANES
    chunk_rows = ny * SUBROWS
    count = 126
    scratch = [
        pltpu.VMEM((w_o.shape[0], half), BF16),
        pltpu.VMEM(w_gate.shape, BF16),
        pltpu.VMEM(w_up.shape, BF16),
        pltpu.VMEM(w_down.shape, BF16),
        pltpu.SemaphoreType.DMA((4,)),
        pltpu.VMEM((nx, chunk_rows, width), F32),
        pltpu.VMEM((nx, chunk_rows, width), F32),
        pltpu.VMEM((6, chunk_rows // 2, width), F32),
        pltpu.VMEM((CORES, chunk_rows, heads_width), F32),
        pltpu.VMEM((ny, SUBROWS, half), F32),
        pltpu.VMEM((6, SUBROWS, half // 2), F32),
        pltpu.VMEM((SUBROWS, LANES), F32),
        pltpu.VMEM((SUBROWS, LANES), F32),
        pltpu.VMEM((CORES, nx, ny, SUBROWS, half), F32),
        pltpu.VMEM((rows, dim), BF16),
        pltpu.VMEM((nx, ny, SUBROWS, half), F32),
        pltpu.VMEM((nx, ny, SUBROWS, half), F32),
        pltpu.VMEM((nx, ny, SUBROWS, half), F32),
        pltpu.VMEM((nx, 6, SUBROWS, half // 2), F32),
        pltpu.VMEM((6, SUBROWS, half // 2), F32),
        pltpu.VMEM((CORES, nx, ny, SUBROWS, half), F32),
        pltpu.SemaphoreType.DMA((count,)),
        pltpu.SemaphoreType.DMA((count,)),
    ]
    return pl.pallas_call(
        functools.partial(rest_kernel, nx, ny, dim),
        out_shape=jax.ShapeDtypeStruct((rows, dim), BF16),
        in_specs=[vmem_spec] * 3 + [any_spec] * 4,
        out_specs=vmem_spec,
        scratch_shapes=scratch,
        compiler_params=pltpu.CompilerParams(collective_id=0, has_side_effects=True, vmem_limit_bytes=50 * 1024 * 1024),
        name="rest_of_layer",
    )(parts, gains, own_x, w_o, w_gate, w_up, w_down)


def solution(mesh):
    row_spec = P('dp', None)
    cache_spec = P('dp', 'sp', 'tp', None)
    new_spec = P('dp', 'tp', None)
    in_specs = (row_spec, P('dp'), cache_spec, cache_spec, P(None), P(None, 'tp'), P(None, 'tp'), P(None, 'tp'), P('tp', None), P(None), P(None, ('tp', 'sp')), P(None, ('tp', 'sp')), P(('tp', 'sp'), None))
    out_specs = (row_spec, cache_spec, cache_spec, new_spec, new_spec)
    nx, ny = mesh.shape["sp"] // CORES, mesh.shape["tp"]

    def local_step(x_in, positions, k_cache, v_cache, attn_gain, w_q, w_k, w_v, w_o, mlp_gain, w_gate, w_up, w_down):
        num_rows, block_len, kv_local, head_dim = k_cache.shape
        dim = x_in.shape[1]
        gains = jnp.stack([attn_gain, mlp_gain]).astype(F32)
        cos_part, sin_part = rotary_tables(positions, head_dim)
        flat = (num_rows, block_len * kv_local, head_dim)
        parts, k_out, v_out, k_new, v_new, own_x = front_of_layer(
            x_in.reshape(nx * ny, SUBROWS, dim), gains, cos_part, sin_part, positions, w_q, w_k, w_v,
            k_cache.reshape(flat), v_cache.reshape(flat), kv_local, ny,
        )
        k_out, v_out = k_out.reshape(k_cache.shape), v_out.reshape(v_cache.shape)
        k_new, v_new = k_new.reshape(num_rows, kv_local, head_dim), v_new.reshape(num_rows, kv_local, head_dim)
        parts = parts.reshape(kv_local, nx, num_rows // nx, parts.shape[-1])
        x_out = rest_of_layer(mesh, parts, own_x, gains, w_o, w_gate, w_up, w_down)
        return x_out, k_out, v_out, k_new, v_new

    return jax.shard_map(local_step, mesh=mesh, in_specs=in_specs, out_specs=out_specs, check_vma=False)
```
